32 devices in a mesh: slab: 16 (over z, x, core), tile: 2 (over y).
Axes of the slice: x: 2, y: 2, z: 4, core: 2. Of those that a mesh axis runs over, the one named last changes fastest.
Arguments:
- features: bfloat16 [16, 2, 512, 128], P('slab', 'tile'), may hold values from -24 to 24
- counts: int32 [16, 2], P('slab', 'tile'), may hold values from 128 to 512, as said below
- rulebook: int32 [16, 2, 27, 512], P('slab', 'tile'), may hold values from 0 to 800, as said below
- face_rows: int32 [16, 2, 4, 64], P('slab', 'tile'), may hold values from 0 to 511, as said below
- conv_one: bfloat16 [27, 128, 128], replicated, may hold values from -0.109375 to 0.109375
- gain_one: float32 [128], replicated, may hold values from 0.5 to 1.5
- shift_one: float32 [128], replicated, may hold values from -0.5 to 0.5
- conv_two: bfloat16 [27, 128, 128], replicated, may hold values from -0.109375 to 0.109375
- gain_two: float32 [128], replicated, may hold values from 0.5 to 1.5
- shift_two: float32 [128], replicated, may hold values from -0.5 to 0.5
Outputs:
- output: bfloat16 [16, 2, 512, 128], P('slab', 'tile')
The draws below stay inside these ranges and needn't reach their ends.
Inputs may be any that keep to these rules, and one draw needn't show every extreme that they name: `counts`: each device's voxels fill its 8 x 8 grid columns with the same number each, between 2 and 8; some device of the highest slab index holds 512. `rulebook`: an entry names the extended-table row that holds the voxel's neighbour at offset k = 9 (dx + 1) + 3 (dy + 1) + (dz + 1) of the submanifold 3x3x3 stencil, or 800 where that cell is inactive or outside the grid; the voxel itself is at offset 13; rows at or past the device's count name 800 at every offset. `face_rows`: lists 0 to 3 hold the device's voxels on its lower and higher face along the first, then the lower and higher face along the second dimension; the j-th voxel of the i-th column along a face stands at position i * 8 + j; unused positions name row 0.
All inputs are finite; a program needn't handle non-finite values.
Results may differ from the reference program's by a relative error of at most 0.0033.
Values may be sent and summed in bfloat16 or wider, within the bound.
A program may use at most 64 MiB of HBM per device.

```python
import math
import jax
import jax.numpy as jnp
from jax import lax

CHANNELS = 128
SIDE = 8
COLUMN = 8
DEPTH = 512
ROWS = 512
FACE = 64
TABLE = 800
N_SLAB = 16
N_TILE = 2


def voxel_layout(key):
    base_key = jax.random.fold_in(key, 11)
    coin_key, pick_key, depth_key = jax.random.split(base_key, 3)
    quarter = COLUMN // 4
    slab_ramp = quarter + (COLUMN - quarter) * jnp.arange(N_SLAB, dtype=jnp.int32) // max(N_SLAB - 1, 1)
    coin_flip = jax.random.randint(coin_key, (N_SLAB, N_TILE), 0, 2)
    per_column = jnp.where(coin_flip == 0, slab_ramp[:, None], quarter).astype(jnp.int32)
    chosen = jax.random.randint(pick_key, (), 0, N_TILE)
    per_column = per_column.at[N_SLAB - 1, chosen].set(COLUMN)
    column_total = N_SLAB * N_TILE * SIDE * SIDE
    depth_keys = jax.random.split(depth_key, column_total)
    shuffled = jax.vmap(lambda one_key: jax.random.permutation(one_key, DEPTH)[:COLUMN])(depth_keys)
    shuffled = shuffled.astype(jnp.int32).reshape(N_SLAB, N_TILE, SIDE, SIDE, COLUMN)
    rank_list = jnp.arange(COLUMN, dtype=jnp.int32)
    full_shape = (N_SLAB, N_TILE, SIDE, SIDE, COLUMN)
    own_count = jnp.broadcast_to(per_column[:, :, None, None, None], full_shape)
    filled = jnp.broadcast_to(rank_list, full_shape) < own_count
    depth_pos = jnp.sort(jnp.where(filled, shuffled, DEPTH + COLUMN), axis=-1)
    local_slab = jnp.broadcast_to(jnp.arange(SIDE, dtype=jnp.int32)[None, None, :, None, None], full_shape)
    local_tile = jnp.broadcast_to(jnp.arange(SIDE, dtype=jnp.int32)[None, None, None, :, None], full_shape)
    slab_index = jnp.broadcast_to(jnp.arange(N_SLAB, dtype=jnp.int32)[:, None, None, None, None], full_shape)
    tile_index = jnp.broadcast_to(jnp.arange(N_TILE, dtype=jnp.int32)[None, :, None, None, None], full_shape)
    slab_cell = slab_index * SIDE + local_slab
    tile_cell = tile_index * SIDE + local_tile
    rank_full = jnp.broadcast_to(rank_list, full_shape)
    occupancy = jnp.full((N_SLAB * SIDE, N_TILE * SIDE, DEPTH), -1, jnp.int32)
    occupancy = occupancy.at[slab_cell, tile_cell, depth_pos].set(rank_full, mode='drop')
    tap_values = []
    for shift_slab in range(-1, 2):
        for shift_tile in range(-1, 2):
            for shift_depth in range(-1, 2):
                near_slab = local_slab + shift_slab
                near_tile = local_tile + shift_tile
                near_depth = depth_pos + shift_depth
                cell_slab = slab_cell + shift_slab
                cell_tile = tile_cell + shift_tile
                inside = (cell_slab >= 0) & (cell_slab < N_SLAB * SIDE) & (cell_tile >= 0) & (cell_tile < N_TILE * SIDE)
                inside = inside & (near_depth >= 0) & (near_depth < DEPTH) & filled
                found_rank = occupancy[jnp.clip(cell_slab, 0, N_SLAB * SIDE - 1), jnp.clip(cell_tile, 0, N_TILE * SIDE - 1), jnp.clip(near_depth, 0, DEPTH - 1)]
                present = inside & (found_rank >= 0)
                in_slab = (near_slab >= 0) & (near_slab < SIDE)
                in_tile = (near_tile >= 0) & (near_tile < SIDE)
                own_index = (near_slab * SIDE + near_tile) * own_count + found_rank
                slab_index_low = ROWS + near_tile * COLUMN + found_rank
                slab_index_high = ROWS + FACE + near_tile * COLUMN + found_rank
                tile_index_low = ROWS + 2 * FACE + (near_slab + 1) * COLUMN + found_rank
                tile_index_high = ROWS + 3 * FACE + 2 * COLUMN + (near_slab + 1) * COLUMN + found_rank
                local_index = jnp.where(in_slab & in_tile, own_index, jnp.where(in_tile, jnp.where(near_slab < 0, slab_index_low, slab_index_high), jnp.where(near_tile < 0, tile_index_low, tile_index_high)))
                tap_values.append(jnp.where(present, local_index, TABLE).astype(jnp.int32))
    stacked = jnp.stack(tap_values, axis=2)
    big_shape = (N_SLAB, N_TILE, 27, SIDE, SIDE, COLUMN)
    row_target = jnp.where(filled, (local_slab * SIDE + local_tile) * own_count + rank_full, ROWS)
    row_target = jnp.broadcast_to(row_target[:, :, None], big_shape)
    slab_target = jnp.broadcast_to(slab_index[:, :, None], big_shape)
    tile_target = jnp.broadcast_to(tile_index[:, :, None], big_shape)
    tap_target = jnp.broadcast_to(jnp.arange(27, dtype=jnp.int32)[None, None, :, None, None, None], big_shape)
    rulebook = jnp.full((N_SLAB, N_TILE, 27, ROWS), TABLE, jnp.int32)
    rulebook = rulebook.at[slab_target, tile_target, tap_target, row_target].set(stacked, mode='drop')
    along_face = jnp.arange(SIDE, dtype=jnp.int32)[None, None, :, None]
    face_rank = rank_list[None, None, None, :]
    face_count = per_column[:, :, None, None]
    face_filled = face_rank < face_count
    slab_lower = (0 * SIDE + along_face) * face_count + face_rank
    slab_upper = ((SIDE - 1) * SIDE + along_face) * face_count + face_rank
    tile_lower = (along_face * SIDE + 0) * face_count + face_rank
    tile_upper = (along_face * SIDE + SIDE - 1) * face_count + face_rank
    face_lists = []
    for face_list in (slab_lower, slab_upper, tile_lower, tile_upper):
        face_lists.append(jnp.where(face_filled, face_list, 0).reshape(N_SLAB, N_TILE, FACE))
    face_rows = jnp.stack(face_lists, axis=2).astype(jnp.int32)
    counts = (per_column * SIDE * SIDE).astype(jnp.int32)
    return (counts, rulebook, face_rows)


def draw_counts(key, part):
    return voxel_layout(key)[0]


def draw_rulebook(key, part):
    return voxel_layout(key)[1]


def draw_face_rows(key, part):
    return voxel_layout(key)[2]


def draw_features(key, part):
    noise_key, row_key, chan_key = jax.random.split(jax.random.fold_in(key, 23), 3)
    array_shape = (N_SLAB, N_TILE, ROWS, CHANNELS)
    row_scale = jnp.exp(jax.random.uniform(row_key, (N_SLAB, N_TILE, ROWS, 1), jnp.float32, math.log(0.3), math.log(3.0)))
    chan_scale = jnp.exp(jax.random.uniform(chan_key, (CHANNELS,), jnp.float32, math.log(0.5), math.log(2.0)))
    base_noise = jnp.clip(jax.random.normal(noise_key, array_shape, jnp.float32), -4.0, 4.0)
    return (base_noise * row_scale * chan_scale).astype(jnp.bfloat16)


def gaussian(own_key, extent, spread, limit, held_as=jnp.bfloat16):
    return jnp.clip(spread * jax.random.normal(own_key, extent, jnp.float32), -limit, limit).astype(held_as)


def setup_inputs(seed: int = 0) -> dict:
    streams_of = jax.random.split(jax.random.key(seed), 11)
    return {
        "features": draw_features(jax.random.fold_in(streams_of[10], 71), 0),
        "counts": draw_counts(jax.random.fold_in(streams_of[10], 71), 0),
        "rulebook": draw_rulebook(jax.random.fold_in(streams_of[10], 71), 0),
        "face_rows": draw_face_rows(jax.random.fold_in(streams_of[10], 71), 0),
        "conv_one": gaussian(streams_of[4], (27, CHANNELS, CHANNELS), (27 * CHANNELS) ** -0.5, 0.109375),
        "gain_one": jnp.clip(1.0 + 0.1 * jax.random.normal(streams_of[5], (CHANNELS,), jnp.float32), 0.5, 1.5),
        "shift_one": jnp.clip(jax.random.uniform(streams_of[6], (CHANNELS,), jnp.float32, -0.5, 0.5), -0.5, 0.5),
        "conv_two": gaussian(streams_of[7], (27, CHANNELS, CHANNELS), (27 * CHANNELS) ** -0.5, 0.109375),
        "gain_two": jnp.clip(1.0 + 0.1 * jax.random.normal(streams_of[8], (CHANNELS,), jnp.float32), 0.5, 1.5),
        "shift_two": jnp.clip(jax.random.uniform(streams_of[9], (CHANNELS,), jnp.float32, -0.5, 0.5), -0.5, 0.5),
    }


EPSILON = 1e-05

def extend(voxel_rows, face_rows):
    picked = jax.vmap(jax.vmap(lambda row_list, positions: row_list[positions]))(voxel_rows, face_rows)
    blank = jnp.zeros_like(picked[:1, :, 0])
    slab_low = jnp.concatenate([blank, picked[:-1, :, 1]], axis=0)
    slab_high = jnp.concatenate([picked[1:, :, 0], blank], axis=0)
    lower_send = jnp.concatenate([slab_low[:, :, :COLUMN], picked[:, :, 2], slab_high[:, :, :COLUMN]], axis=2)
    upper_send = jnp.concatenate([slab_low[:, :, FACE - COLUMN:], picked[:, :, 3], slab_high[:, :, FACE - COLUMN:]], axis=2)
    edge_rows = jnp.zeros_like(lower_send[:, :1])
    tile_low = jnp.concatenate([edge_rows, upper_send[:, :-1]], axis=1)
    tile_high = jnp.concatenate([lower_send[:, 1:], edge_rows], axis=1)
    zero_row = jnp.zeros_like(voxel_rows[:, :, :1])
    return jnp.concatenate([voxel_rows, slab_low, slab_high, tile_low, tile_high, zero_row], axis=2)

def convolve_all(lookup, rulebook, weight):
    device_count = N_SLAB * N_TILE
    flat_weight = weight.astype(jnp.float32).reshape(27 * CHANNELS, CHANNELS)
    tables = lookup.reshape(device_count, TABLE + 1, CHANNELS)
    indices = rulebook.reshape(device_count, 27, ROWS)

    def one_device(pair):
        table_rows, tap_rows = pair
        gathered = table_rows[tap_rows.T].reshape(ROWS, 27 * CHANNELS).astype(jnp.float32)
        return jnp.dot(gathered, flat_weight, preferred_element_type=jnp.float32)
    result = lax.map(one_device, (tables, indices))
    return result.reshape(N_SLAB, N_TILE, ROWS, CHANNELS)

def normalize(conv_out, live_mask, voxel_total, gain, shift):
    average = lax.optimization_barrier(jnp.sum(conv_out * live_mask, axis=(0, 1, 2))) / voxel_total
    centred = (conv_out - average) * live_mask
    variance = lax.optimization_barrier(jnp.sum(centred * centred, axis=(0, 1, 2))) / voxel_total
    return (conv_out - average) / jnp.sqrt(variance + EPSILON) * gain + shift

def reference(features, counts, rulebook, face_rows, conv_one, gain_one, shift_one, conv_two, gain_two, shift_two):
    live_mask = (jnp.arange(ROWS, dtype=jnp.int32)[None, None, :] < counts[:, :, None]).astype(jnp.float32)[..., None]
    voxel_total = jnp.sum(counts).astype(jnp.float32)
    first = convolve_all(extend(features, face_rows), rulebook, conv_one)
    hidden = (live_mask * jnp.maximum(normalize(first, live_mask, voxel_total, gain_one, shift_one), 0.0)).astype(jnp.bfloat16)
    second = convolve_all(extend(hidden, face_rows), rulebook, conv_two)
    summed = normalize(second, live_mask, voxel_total, gain_two, shift_two) + features.astype(jnp.float32)
    return (live_mask * jnp.maximum(summed, 0.0)).astype(jnp.bfloat16)
```

```python
from functools import partial

import jax
import jax.numpy as jnp
from jax import lax
from jax.experimental import pallas as pl
from jax.experimental.pallas import tpu as pltpu
from jax.sharding import PartitionSpec as P

SIDE = 8
EPSILON = 1e-05
MESH = pl.DeviceIdType.MESH
BLOCK = 256
PIECE = 16
F32 = jnp.float32
BF16 = jnp.bfloat16


def transfers(face_len):
    low, high = 0, face_len
    edge = face_len - PIECE
    end = PIECE + face_len
    return (
        (1, 0, high, face_len, 0, 0),
        (-1, 0, low, face_len, 0, face_len),
        (0, 1, 3 * face_len, face_len, 1, PIECE),
        (0, -1, 2 * face_len, face_len, 2, PIECE),
        (1, 1, high + edge, PIECE, 1, 0),
        (-1, 1, low + edge, PIECE, 1, end),
        (1, -1, high, PIECE, 2, 0),
        (-1, -1, low, PIECE, 2, end),
    )


def block_kernel(
    n_slab,
    n_tile,
    feat_ref,
    count_ref,
    rule_ref,
    face_ref,
    gain_one_ref,
    shift_one_ref,
    gain_two_ref,
    shift_two_ref,
    conv_one_ref,
    conv_two_ref,
    out_ref,
    weight_ref,
    weight_t_ref,
    onehot_ref,
    part_ref,
    face_hot_ref,
    square_ref,
    send_ref,
    halo_ref,
    lhs_ref,
    picked_ref,
    stats_ref,
    weight_sem,
    send_sem,
    recv_sem,
    stat_send_sem,
    stat_recv_sem,
):
    rows, channels = feat_ref.shape
    taps = rule_ref.shape[0]
    face_len = face_ref.shape[1]
    column = face_len // SIDE
    n_dev = n_slab * n_tile
    blocks = rows // BLOCK
    group = taps // 3
    slab = lax.axis_index("slab")
    tile = lax.axis_index("tile")
    me = slab * n_tile + tile

    weight_copies = [
        pltpu.make_async_copy(src, weight_ref.at[i], weight_sem.at[i])
        for i, src in enumerate((conv_one_ref, conv_two_ref))
    ]
    for copy in weight_copies:
        copy.start()
    halo_ref[...] = jnp.zeros_like(halo_ref)

    def peer_of(step):
        peer = lax.rem(me + step, n_dev)
        return {"slab": peer // n_tile, "tile": lax.rem(peer, n_tile)}

    barrier = pltpu.get_barrier_semaphore()

    def greet(step, carry):
        pl.semaphore_signal(barrier, inc=1, device_id=peer_of(step), device_id_type=MESH)
        return carry

    lax.fori_loop(1, n_dev, greet, 0)

    def halo(which, start):
        for j, (ds, dt, first, size, buffer, place) in enumerate(transfers(face_len)):
            copy = pltpu.make_async_remote_copy(
                src_ref=send_ref.at[which, pl.ds(first, size)],
                dst_ref=halo_ref.at[which, buffer, pl.ds(place, size)],
                send_sem=send_sem.at[which, j],
                recv_sem=recv_sem.at[which, j],
                device_id={"slab": slab + ds, "tile": tile + dt},
                device_id_type=MESH,
            )
            sends, receives = True, True
            if ds > 0:
                sends, receives = slab < n_slab - 1, slab > 0
            elif ds < 0:
                sends, receives = slab > 0, slab < n_slab - 1
            if dt > 0:
                sends, receives = sends & (tile < n_tile - 1), receives & (tile > 0)
            elif dt < 0:
                sends, receives = sends & (tile > 0), receives & (tile < n_tile - 1)
            if start:
                pl.when(sends)(copy.start)
            else:
                pl.when(receives)(copy.wait_recv)
                pl.when(sends)(copy.wait_send)

    square_ref[...] = jnp.zeros_like(square_ref)
    square_ref[0:4, 0:face_len] = face_ref[...].astype(F32)
    face_cols = square_ref[...].T
    lane_rows = lax.broadcasted_iota(jnp.int32, (face_len, rows), 1)
    for k in range(4):
        wanted = face_cols[0:face_len, k : k + 1].astype(jnp.int32)
        face_hot_ref[k * face_len : (k + 1) * face_len, :] = jnp.where(
            lane_rows == wanted, 1.0, 0.0
        ).astype(BF16)

    feat = feat_ref[...]
    send_ref[0] = jnp.dot(face_hot_ref[...], feat, preferred_element_type=F32).astype(BF16)
    pl.semaphore_wait(barrier, n_dev - 1)
    halo(0, True)

    rule = rule_ref[...]
    tile_len = face_len + 2 * column
    below = rows + 2 * face_len
    above = below + tile_len
    q_low = rule - below
    q_high = rule - above
    base = 2 * face_len + PIECE - column
    skip = PIECE - column
    place_low = base + q_low + jnp.where(q_low >= column + face_len, skip, 0)
    place_high = base + q_high - jnp.where(q_high < column, skip, 0)
    place = jnp.where(
        rule < rows,
        rule & (BLOCK - 1),
        jnp.where(
            rule < below, rule - rows, jnp.where(rule < above, place_low, place_high)
        ),
    )
    part = jnp.where(
        rule < rows, rule // BLOCK, jnp.where(rule < above + tile_len, blocks, blocks + 1)
    )
    position = lax.broadcasted_iota(jnp.int32, (BLOCK, rows), 0)
    for k in range(taps):
        part_ref[k] = part[k : k + 1]
        onehot_ref[k] = jnp.where(position == place[k : k + 1], 1.0, 0.0).astype(BF16)

    def load_local(values):
        for b in range(blocks):
            turned = values[b * BLOCK : (b + 1) * BLOCK].T
            for y in range(3):
                lhs_ref[y, b * channels : (b + 1) * channels, :] = turned

    def load_halo(which):
        turned = [halo_ref[which, i].T for i in range(3)]
        low = blocks * channels
        half = BLOCK // 2
        for y, other in ((0, turned[1]), (1, None), (2, turned[2])):
            lhs_ref[y, low:, 0:half] = turned[0]
            lhs_ref[y, low:, half:] = jnp.zeros_like(turned[0]) if other is None else other

    load_local(feat)
    for i in range(2):
        weight_copies[i].wait()
        for x in range(3):
            weight_t_ref[i, x] = weight_ref[i, x * group * channels : (x + 1) * group * channels, :].T

    def convolve(which):
        def one(x, total):
            for j in range(group):
                tap = x * group + j
                found = jnp.dot(
                    lhs_ref[j // 3], onehot_ref[tap], preferred_element_type=F32
                )
                home = part_ref[tap]
                value = jnp.zeros((channels, rows), F32)
                for b in range(blocks + 1):
                    value = jnp.where(
                        home == b, found[b * channels : (b + 1) * channels], value
                    )
                picked_ref[j * channels : (j + 1) * channels, :] = value.astype(BF16)
            return total + jnp.dot(
                weight_t_ref[which, x], picked_ref[...], preferred_element_type=F32
            )

        return lax.fori_loop(0, 3, one, jnp.zeros((channels, rows), F32))

    count = count_ref[0, 0]
    live = (lax.broadcasted_iota(jnp.int32, (rows, 1), 0) < count).astype(F32)

    def stat_copy(which, target):
        return pltpu.make_async_remote_copy(
            src_ref=stats_ref.at[which, me],
            dst_ref=stats_ref.at[which, me],
            send_sem=stat_send_sem.at[which],
            recv_sem=stat_recv_sem.at[which],
            device_id=target,
            device_id_type=MESH,
        )

    def affine(which, values, gain_ref, shift_ref):
        kept = values * live
        stats_ref[which, me] = jnp.concatenate(
            [
                jnp.sum(kept, axis=0, keepdims=True),
                jnp.sum(kept * values, axis=0, keepdims=True),
                jnp.full((2, channels), count.astype(F32)),
            ],
            axis=0,
        )

        def tell(step, carry):
            stat_copy(which, peer_of(step)).start()
            return carry

        lax.fori_loop(1, n_dev, tell, 0)
        others = stats_ref.at[which, pl.ds(0, n_dev - 1)]
        pltpu.make_async_copy(others, others, stat_recv_sem.at[which]).wait()
        pltpu.make_async_copy(others, others, stat_send_sem.at[which]).wait()
        total = jnp.sum(stats_ref[which], axis=0)
        average = total[0:1] / total[2:3]
        variance = total[1:2] / total[2:3] - average * average
        scale = lax.rsqrt(variance + EPSILON) * gain_ref[...]
        return (values - average) * scale + shift_ref[...]

    halo(0, False)
    load_halo(0)
    first = convolve(0).T
    hidden = (live * jnp.maximum(affine(0, first, gain_one_ref, shift_one_ref), 0.0)).astype(BF16)
    send_ref[1] = jnp.dot(face_hot_ref[...], hidden, preferred_element_type=F32).astype(BF16)
    halo(1, True)
    load_local(hidden)
    halo(1, False)
    load_halo(1)
    second = convolve(1).T
    summed = affine(1, second, gain_two_ref, shift_two_ref) + feat.astype(F32)
    out_ref[...] = (live * jnp.maximum(summed, 0.0)).astype(BF16)


def per_device(
    n_slab,
    n_tile,
    features,
    counts,
    rulebook,
    face_rows,
    conv_one,
    gain_one,
    shift_one,
    conv_two,
    gain_two,
    shift_two,
):
    rows, channels = features.shape[2:]
    taps = rulebook.shape[2]
    faces, face_len = face_rows.shape[2:]
    blocks = rows // BLOCK
    vmem = pl.BlockSpec(memory_space=pltpu.VMEM)
    smem = pl.BlockSpec(memory_space=pltpu.SMEM)
    hbm = pl.BlockSpec(memory_space=pl.ANY)
    group = taps // 3 * channels
    output = pl.pallas_call(
        partial(block_kernel, n_slab, n_tile),
        out_shape=jax.ShapeDtypeStruct((rows, channels), features.dtype),
        in_specs=[vmem, smem, vmem, vmem, vmem, vmem, vmem, vmem, hbm, hbm],
        out_specs=vmem,
        scratch_shapes=[
            pltpu.VMEM((2, taps * channels, channels), BF16),
            pltpu.VMEM((2, 3, channels, group), BF16),
            pltpu.VMEM((taps, BLOCK, rows), BF16),
            pltpu.VMEM((taps, 1, rows), jnp.int32),
            pltpu.VMEM((faces * face_len, rows), BF16),
            pltpu.VMEM((128, 128), F32),
            pltpu.VMEM((2, faces * face_len, channels), BF16),
            pltpu.VMEM((2, 3, BLOCK // 2, channels), BF16),
            pltpu.VMEM((3, (blocks + 1) * channels, BLOCK), BF16),
            pltpu.VMEM((group, rows), BF16),
            pltpu.VMEM((2, n_slab * n_tile, 4, channels), F32),
            pltpu.SemaphoreType.DMA((2,)),
            pltpu.SemaphoreType.DMA((2, 8)),
            pltpu.SemaphoreType.DMA((2, 8)),
            pltpu.SemaphoreType.DMA((2,)),
            pltpu.SemaphoreType.DMA((2,)),
        ],
        compiler_params=pltpu.CompilerParams(
            collective_id=0, has_side_effects=True, vmem_limit_bytes=50 * 1024 * 1024
        ),
    )(
        features[0, 0],
        counts,
        rulebook[0, 0],
        face_rows[0, 0],
        gain_one[None],
        shift_one[None],
        gain_two[None],
        shift_two[None],
        conv_one.reshape(taps * channels, channels),
        conv_two.reshape(taps * channels, channels),
    )
    return output[None, None]


def solution(mesh):
    placed = (
        P("slab", "tile", None, None),
        P("slab", "tile"),
        P("slab", "tile", None, None),
        P("slab", "tile", None, None),
        P(),
        P(),
        P(),
        P(),
        P(),
        P(),
    )
    return jax.shard_map(
        partial(per_device, mesh.shape["slab"], mesh.shape["tile"]),
        mesh=mesh,
        in_specs=placed,
        out_specs=P("slab", "tile", None, None),
        check_vma=False,
    )
```

```python
from functools import partial

import jax
import jax.numpy as jnp
from jax import lax
from jax.experimental import pallas as pl
from jax.experimental.pallas import tpu as pltpu
from jax.sharding import PartitionSpec as P

SIDE = 8
EPSILON = 1e-05
MESH = pl.DeviceIdType.MESH
BLOCK = 256
PIECE = 16
F32 = jnp.float32
BF16 = jnp.bfloat16


def transfers(face_len):
    low, high = 0, face_len
    edge = face_len - PIECE
    end = PIECE + face_len
    return (
        (1, 0, high, face_len, 0, 0),
        (-1, 0, low, face_len, 0, face_len),
        (0, 1, 3 * face_len, face_len, 1, PIECE),
        (0, -1, 2 * face_len, face_len, 2, PIECE),
        (1, 1, high + edge, PIECE, 1, 0),
        (-1, 1, low + edge, PIECE, 1, end),
        (1, -1, high, PIECE, 2, 0),
        (-1, -1, low, PIECE, 2, end),
    )


def block_kernel(
    n_slab,
    n_tile,
    feat_hbm,
    count_ref,
    rule_hbm,
    face_hbm,
    gain_one_ref,
    shift_one_ref,
    gain_two_ref,
    shift_two_ref,
    conv_one_ref,
    conv_two_ref,
    out_ref,
    feat_ref,
    rule_ref,
    face_ref,
    weight_ref,
    weight_t_ref,
    onehot_ref,
    part_ref,
    face_hot_ref,
    square_ref,
    send_ref,
    wide_send_ref,
    halo_ref,
    wide_halo_ref,
    lhs_ref,
    picked_ref,
    stats_ref,
    input_sem,
    weight_sem,
    send_sem,
    recv_sem,
    stat_send_sem,
    stat_recv_sem,
):
    rows, channels = feat_ref.shape
    taps = rule_ref.shape[0]
    face_len = face_ref.shape[1]
    column = face_len // SIDE
    n_dev = n_slab * n_tile
    blocks = rows // BLOCK
    group = taps // 3
    slab = lax.axis_index("slab")
    tile = lax.axis_index("tile")
    me = slab * n_tile + tile

    input_copies = [
        pltpu.make_async_copy(src, dst, input_sem.at[i])
        for i, (src, dst) in enumerate(
            ((feat_hbm, feat_ref), (face_hbm, face_ref), (rule_hbm, rule_ref))
        )
    ]
    for copy in input_copies:
        copy.start()
    weight_copies = [
        pltpu.make_async_copy(src, weight_ref.at[i], weight_sem.at[i])
        for i, src in enumerate((conv_one_ref, conv_two_ref))
    ]
    for copy in weight_copies:
        copy.start()
    halo_ref[...] = jnp.zeros_like(halo_ref)
    wide_halo_ref[...] = jnp.zeros_like(wide_halo_ref)

    def peer_of(step):
        peer = lax.rem(me + step, n_dev)
        return {"slab": peer // n_tile, "tile": lax.rem(peer, n_tile)}

    barrier = pltpu.get_barrier_semaphore()

    def greet(step, carry):
        pl.semaphore_signal(barrier, inc=1, device_id=peer_of(step), device_id_type=MESH)
        return carry

    lax.fori_loop(1, n_dev, greet, 0)

    def halo(which, start):
        source, target = ((send_ref, halo_ref), (wide_send_ref, wide_halo_ref))[which]
        for j, (ds, dt, first, size, buffer, place) in enumerate(transfers(face_len)):
            copy = pltpu.make_async_remote_copy(
                src_ref=source.at[pl.ds(first, size)],
                dst_ref=target.at[buffer, pl.ds(place, size)],
                send_sem=send_sem.at[which, j],
                recv_sem=recv_sem.at[which, j],
                device_id={"slab": slab + ds, "tile": tile + dt},
                device_id_type=MESH,
            )
            sends, receives = True, True
            if ds > 0:
                sends, receives = slab < n_slab - 1, slab > 0
            elif ds < 0:
                sends, receives = slab > 0, slab < n_slab - 1
            if dt > 0:
                sends, receives = sends & (tile < n_tile - 1), receives & (tile > 0)
            elif dt < 0:
                sends, receives = sends & (tile > 0), receives & (tile < n_tile - 1)
            if start:
                pl.when(sends)(copy.start)
            else:
                pl.when(receives)(copy.wait_recv)
                pl.when(sends)(copy.wait_send)

    input_copies[1].wait()
    square_ref[...] = jnp.zeros_like(square_ref)
    square_ref[0:4, 0:face_len] = face_ref[...].astype(F32)
    face_cols = square_ref[...].T
    lane_rows = lax.broadcasted_iota(jnp.int32, (face_len, rows), 1)
    for k in range(4):
        wanted = face_cols[0:face_len, k : k + 1].astype(jnp.int32)
        face_hot_ref[k * face_len : (k + 1) * face_len, :] = jnp.where(
            lane_rows == wanted, 1.0, 0.0
        ).astype(BF16)

    input_copies[0].wait()
    feat = feat_ref[...]
    send_ref[...] = jnp.dot(face_hot_ref[...], feat, preferred_element_type=F32).astype(BF16)

    input_copies[2].wait()
    rule = rule_ref[...]
    tile_len = face_len + 2 * column
    below = rows + 2 * face_len
    above = below + tile_len
    q_low = rule - below
    q_high = rule - above
    base = 2 * face_len + PIECE - column
    skip = PIECE - column
    place_low = base + q_low + jnp.where(q_low >= column + face_len, skip, 0)
    place_high = base + q_high - jnp.where(q_high < column, skip, 0)
    place = jnp.where(
        rule < rows,
        rule & (BLOCK - 1),
        jnp.where(
            rule < below, rule - rows, jnp.where(rule < above, place_low, place_high)
        ),
    )
    part = jnp.where(
        rule < rows, rule // BLOCK, jnp.where(rule < above + tile_len, blocks, blocks + 1)
    )
    part_ref[...] = part
    position = lax.broadcasted_iota(jnp.int32, (BLOCK, rows), 0)
    for k in range(taps):
        onehot_ref[k] = jnp.where(position == place[k], 1.0, 0.0).astype(BF16)

    pl.semaphore_wait(barrier, n_dev - 1)
    halo(0, True)

    def load_local(values):
        for b in range(blocks):
            turned = values[b * BLOCK : (b + 1) * BLOCK].T
            for y in range(3):
                lhs_ref[y, b * channels : (b + 1) * channels, :] = turned

    def load_halo(pieces):
        turned = [piece.T for piece in pieces]
        low = blocks * channels
        half = BLOCK // 2
        for y, other in ((0, turned[1]), (1, None), (2, turned[2])):
            lhs_ref[y, low:, 0:half] = turned[0]
            lhs_ref[y, low:, half:] = jnp.zeros_like(turned[0]) if other is None else other

    load_local(feat)
    for i in range(2):
        weight_copies[i].wait()
        for x in range(3):
            weight_t_ref[i, x] = weight_ref[i, x * group * channels : (x + 1) * group * channels, :].T

    def choose(home, found, value, chosen):
        for i, b in enumerate(chosen):
            value = jnp.where(home == b, found[i * channels : (i + 1) * channels], value)
        return value

    def pick_local(tap, carry):
        found = jnp.dot(
            lhs_ref[0, 0 : blocks * channels], onehot_ref[tap], preferred_element_type=F32
        )
        value = choose(part_ref[tap], found, jnp.zeros((channels, rows), F32), range(blocks))
        picked_ref[tap] = value.astype(BF16)
        return carry

    def convolve(which, picked):
        def one(x, total):
            for j in range(group):
                tap = x * group + j
                home = part_ref[tap]
                if picked:
                    found = jnp.dot(
                        lhs_ref[j // 3, blocks * channels :],
                        onehot_ref[tap],
                        preferred_element_type=F32,
                    )
                    value = choose(home, found, picked_ref[tap].astype(F32), (blocks,))
                else:
                    found = jnp.dot(
                        lhs_ref[j // 3], onehot_ref[tap], preferred_element_type=F32
                    )
                    value = choose(
                        home, found, jnp.zeros((channels, rows), F32), range(blocks + 1)
                    )
                picked_ref[tap] = value.astype(BF16)
            taken = picked_ref[pl.ds(x * group, group)].reshape(group * channels, rows)
            return total + jnp.dot(weight_t_ref[which, x], taken, preferred_element_type=F32)

        return lax.fori_loop(0, 3, one, jnp.zeros((channels, rows), F32))

    count = count_ref[0, 0]
    live = (lax.broadcasted_iota(jnp.int32, (rows, 1), 0) < count).astype(F32)

    def stat_copy(which, target):
        return pltpu.make_async_remote_copy(
            src_ref=stats_ref.at[which, me],
            dst_ref=stats_ref.at[which, me],
            send_sem=stat_send_sem.at[which],
            recv_sem=stat_recv_sem.at[which],
            device_id=target,
            device_id_type=MESH,
        )

    def tell_sums(which, values):
        kept = values * live
        stats_ref[which, me] = jnp.concatenate(
            [
                jnp.sum(kept, axis=0, keepdims=True),
                jnp.sum(kept * values, axis=0, keepdims=True),
                jnp.full((2, channels), count.astype(F32)),
            ],
            axis=0,
        )

        def tell(step, carry):
            stat_copy(which, peer_of(step)).start()
            return carry

        lax.fori_loop(1, n_dev, tell, 0)

    def affine(which, gain_ref, shift_ref):
        others = stats_ref.at[which, pl.ds(0, n_dev - 1)]
        pltpu.make_async_copy(others, others, stat_recv_sem.at[which]).wait()
        pltpu.make_async_copy(others, others, stat_send_sem.at[which]).wait()
        total = jnp.sum(stats_ref[which], axis=0)
        average = total[0:1] / total[2:3]
        variance = total[1:2] / total[2:3] - average * average
        scale = lax.rsqrt(variance + EPSILON) * gain_ref[...]
        return lambda values: (values - average) * scale + shift_ref[...]

    lax.fori_loop(0, taps, pick_local, 0, unroll=3)
    halo(0, False)
    load_halo([halo_ref[i] for i in range(3)])
    first = convolve(0, True).T
    tell_sums(0, first)
    coarse = first.astype(BF16)
    fine = (first - coarse.astype(F32)).astype(BF16)
    both = jnp.dot(
        face_hot_ref[...],
        jnp.concatenate([coarse, fine], axis=1),
        preferred_element_type=F32,
    )
    wide_send_ref[...] = both[:, 0:channels] + both[:, channels:]
    halo(1, True)
    norm_one = affine(0, gain_one_ref, shift_one_ref)
    load_local((live * jnp.maximum(norm_one(first), 0.0)).astype(BF16))
    halo(1, False)
    load_halo([jnp.maximum(norm_one(wide_halo_ref[i]), 0.0).astype(BF16) for i in range(3)])
    second = convolve(1, False).T
    tell_sums(1, second)
    norm_two = affine(1, gain_two_ref, shift_two_ref)
    summed = norm_two(second) + feat_ref[...].astype(F32)
    out_ref[...] = (live * jnp.maximum(summed, 0.0)).astype(BF16)


def per_device(
    n_slab,
    n_tile,
    features,
    counts,
    rulebook,
    face_rows,
    conv_one,
    gain_one,
    shift_one,
    conv_two,
    gain_two,
    shift_two,
):
    rows, channels = features.shape[2:]
    taps = rulebook.shape[2]
    faces, face_len = face_rows.shape[2:]
    blocks = rows // BLOCK
    smem = pl.BlockSpec(memory_space=pltpu.SMEM)
    vmem = pl.BlockSpec(memory_space=pltpu.VMEM)
    hbm = pl.BlockSpec(memory_space=pltpu.HBM)
    group = taps // 3 * channels
    output = pl.pallas_call(
        partial(block_kernel, n_slab, n_tile),
        out_shape=jax.ShapeDtypeStruct((rows, channels), features.dtype),
        in_specs=[hbm, smem, hbm, hbm, vmem, vmem, vmem, vmem, hbm, hbm],
        out_specs=vmem,
        scratch_shapes=[
            pltpu.VMEM((rows, channels), BF16),
            pltpu.VMEM((taps, 1, rows), jnp.int32),
            pltpu.VMEM((faces, face_len), jnp.int32),
            pltpu.VMEM((2, taps * channels, channels), BF16),
            pltpu.VMEM((2, 3, channels, group), BF16),
            pltpu.VMEM((taps, BLOCK, rows), BF16),
            pltpu.VMEM((taps, 1, rows), jnp.int32),
            pltpu.VMEM((faces * face_len, rows), BF16),
            pltpu.VMEM((128, 128), F32),
            pltpu.VMEM((faces * face_len, channels), BF16),
            pltpu.VMEM((faces * face_len, channels), F32),
            pltpu.VMEM((3, BLOCK // 2, channels), BF16),
            pltpu.VMEM((3, BLOCK // 2, channels), F32),
            pltpu.VMEM((3, (blocks + 1) * channels, BLOCK), BF16),
            pltpu.VMEM((taps, channels, rows), BF16),
            pltpu.VMEM((2, n_slab * n_tile, 4, channels), F32),
            pltpu.SemaphoreType.DMA((3,)),
            pltpu.SemaphoreType.DMA((2,)),
            pltpu.SemaphoreType.DMA((2, 8)),
            pltpu.SemaphoreType.DMA((2, 8)),
            pltpu.SemaphoreType.DMA((2,)),
            pltpu.SemaphoreType.DMA((2,)),
        ],
        compiler_params=pltpu.CompilerParams(
            collective_id=0, has_side_effects=True, vmem_limit_bytes=55500000
        ),
    )(
        features[0, 0],
        counts,
        rulebook.reshape(taps, 1, rows),
        face_rows[0, 0],
        gain_one[None],
        shift_one[None],
        gain_two[None],
        shift_two[None],
        conv_one.reshape(taps * channels, channels),
        conv_two.reshape(taps * channels, channels),
    )
    return output[None, None]


def solution(mesh):
    placed = (
        P("slab", "tile", None, None),
        P("slab", "tile"),
        P("slab", "tile", None, None),
        P("slab", "tile", None, None),
        P(),
        P(),
        P(),
        P(),
        P(),
        P(),
    )
    return jax.shard_map(
        partial(per_device, mesh.shape["slab"], mesh.shape["tile"]),
        mesh=mesh,
        in_specs=placed,
        out_specs=P("slab", "tile", None, None),
        check_vma=False,
    )
```

```python
from functools import partial

import jax
import jax.numpy as jnp
from jax import lax
from jax.experimental import pallas as pl
from jax.experimental.pallas import tpu as pltpu
from jax.sharding import PartitionSpec as P

SIDE = 8
EPSILON = 1e-05
MESH = pl.DeviceIdType.MESH
BLOCK = 256
PIECE = 16
F32 = jnp.float32
BF16 = jnp.bfloat16


def transfers(face_len):
    low, high = 0, face_len
    edge = face_len - PIECE
    end = PIECE + face_len
    return (
        (1, 0, high, face_len, 0, 0),
        (-1, 0, low, face_len, 0, face_len),
        (0, 1, 3 * face_len, face_len, 1, PIECE),
        (0, -1, 2 * face_len, face_len, 2, PIECE),
        (1, 1, high + edge, PIECE, 1, 0),
        (-1, 1, low + edge, PIECE, 1, end),
        (1, -1, high, PIECE, 2, 0),
        (-1, -1, low, PIECE, 2, end),
    )


def block_kernel(
    n_slab,
    n_tile,
    feat_hbm,
    count_ref,
    rule_hbm,
    face_hbm,
    gain_one_hbm,
    shift_one_hbm,
    gain_two_hbm,
    shift_two_hbm,
    conv_one_ref,
    conv_two_ref,
    out_ref,
    feat_ref,
    rule_ref,
    face_ref,
    gain_one_ref,
    shift_one_ref,
    gain_two_ref,
    shift_two_ref,
    weight_ref,
    weight_t_ref,
    onehot_ref,
    part_ref,
    face_hot_ref,
    square_ref,
    send_ref,
    wide_send_ref,
    halo_ref,
    wide_halo_ref,
    lhs_ref,
    picked_ref,
    stats_ref,
    counts_ref,
    input_sem,
    send_sem,
    recv_sem,
    stat_send_sem,
    stat_recv_sem,
):
    rows, channels = feat_ref.shape
    taps = rule_ref.shape[0]
    face_len = face_ref.shape[1]
    column = face_len // SIDE
    n_dev = n_slab * n_tile
    blocks = rows // BLOCK
    group = taps // 3
    ahead = 2
    slab = lax.axis_index("slab")
    tile = lax.axis_index("tile")
    me = slab * n_tile + tile

    def fetch(i, src, dst):
        return pltpu.make_async_copy(src, dst, input_sem.at[i])

    input_copies = [
        fetch(0, feat_hbm, feat_ref),
        fetch(1, face_hbm, face_ref),
        fetch(2, rule_hbm, rule_ref),
    ]
    affine_copies = [
        fetch(3, gain_one_hbm, gain_one_ref),
        fetch(4, shift_one_hbm, shift_one_ref),
        fetch(5, gain_two_hbm, gain_two_ref),
        fetch(6, shift_two_hbm, shift_two_ref),
    ]
    weight_copies = [
        fetch(7, conv_one_ref, weight_ref.at[0]),
        fetch(8, conv_two_ref, weight_ref.at[1]),
    ]
    for copy in (input_copies[1], input_copies[0], input_copies[2]):
        copy.start()
    halo_ref[...] = jnp.zeros_like(halo_ref)
    wide_halo_ref[...] = jnp.zeros_like(wide_halo_ref)

    def wrapped(place, step, size):
        moved = place + step
        return jnp.where(moved >= size, moved - size, moved)

    def each_peer(act):
        for j in range(n_tile):
            other = tile if j == 0 else wrapped(tile, j, n_tile)

            def visit(i, carry):
                act({"slab": wrapped(slab, i, n_slab), "tile": other})
                return carry

            first = 1 if j == 0 else 0
            lax.fori_loop(first, n_slab, visit, 0, unroll=n_slab <= 16)

    barrier = pltpu.get_barrier_semaphore()

    each_peer(
        lambda peer: pl.semaphore_signal(
            barrier, inc=1, device_id=peer, device_id_type=MESH
        )
    )
    for copy in weight_copies + affine_copies:
        copy.start()

    def halo(which, start):
        source, target = ((send_ref, halo_ref), (wide_send_ref, wide_halo_ref))[which]
        for j, (ds, dt, first, size, buffer, place) in enumerate(transfers(face_len)):
            copy = pltpu.make_async_remote_copy(
                src_ref=source.at[pl.ds(first, size)],
                dst_ref=target.at[buffer, pl.ds(place, size)],
                send_sem=send_sem.at[which, j],
                recv_sem=recv_sem.at[which, j],
                device_id={"slab": slab + ds, "tile": tile + dt},
                device_id_type=MESH,
            )
            sends, receives = True, True
            if ds > 0:
                sends, receives = slab < n_slab - 1, slab > 0
            elif ds < 0:
                sends, receives = slab > 0, slab < n_slab - 1
            if dt > 0:
                sends, receives = sends & (tile < n_tile - 1), receives & (tile > 0)
            elif dt < 0:
                sends, receives = sends & (tile > 0), receives & (tile < n_tile - 1)
            if start:
                pl.when(sends)(copy.start)
            else:
                pl.when(receives)(copy.wait_recv)
                pl.when(sends)(copy.wait_send)

    input_copies[1].wait()
    square_ref[...] = jnp.zeros_like(square_ref)
    square_ref[0:4, 0:face_len] = face_ref[...].astype(F32)
    face_cols = square_ref[...].T
    lane_rows = lax.broadcasted_iota(jnp.int32, (face_len, rows), 1)
    for k in range(4):
        wanted = face_cols[0:face_len, k : k + 1].astype(jnp.int32)
        face_hot_ref[k * face_len : (k + 1) * face_len, :] = jnp.where(
            lane_rows == wanted, 1.0, 0.0
        ).astype(BF16)

    input_copies[0].wait()
    feat = feat_ref[...]
    send_ref[...] = jnp.dot(face_hot_ref[...], feat, preferred_element_type=F32).astype(BF16)

    input_copies[2].wait()
    rule = rule_ref[...]
    tile_len = face_len + 2 * column
    below = rows + 2 * face_len
    above = below + tile_len
    q_low = rule - below
    q_high = rule - above
    base = 2 * face_len + PIECE - column
    skip = PIECE - column
    place_low = base + q_low + jnp.where(q_low >= column + face_len, skip, 0)
    place_high = base + q_high - jnp.where(q_high < column, skip, 0)
    place = jnp.where(
        rule < rows,
        rule & (BLOCK - 1),
        jnp.where(
            rule < below, rule - rows, jnp.where(rule < above, place_low, place_high)
        ),
    )
    part = jnp.where(
        rule < rows, rule // BLOCK, jnp.where(rule < above + tile_len, blocks, blocks + 1)
    )
    part_ref[...] = part
    position = lax.broadcasted_iota(jnp.int32, (BLOCK, rows), 0).astype(F32).astype(BF16)
    place = place.astype(F32).astype(BF16)
    one, none = jnp.ones((BLOCK, rows), BF16), jnp.zeros((BLOCK, rows), BF16)
    for k in range(taps):
        onehot_ref[k] = jnp.where(position == place[k], one, none)

    count = count_ref[0, 0]
    live = (lax.broadcasted_iota(jnp.int32, (rows, 1), 0) < count).astype(F32)

    def share(which, buffer):
        mine = buffer.at[me]
        each_peer(
            lambda peer: pltpu.make_async_remote_copy(
                src_ref=mine,
                dst_ref=mine,
                send_sem=stat_send_sem.at[which],
                recv_sem=stat_recv_sem.at[which],
                device_id=peer,
                device_id_type=MESH,
            ).start()
        )

    def shared(which, buffer):
        others = buffer.at[pl.ds(0, n_dev - 1)]
        pltpu.make_async_copy(others, others, stat_recv_sem.at[which]).wait()
        pltpu.make_async_copy(others, others, stat_send_sem.at[which]).wait()
        return jnp.sum(buffer[...], axis=0)

    counts_ref[me] = jnp.full((1, channels), count.astype(F32))
    pl.semaphore_wait(barrier, n_dev - 1)
    halo(0, True)
    share(2, counts_ref)

    def load_local(values):
        for b in range(blocks):
            turned = values[b * BLOCK : (b + 1) * BLOCK].T
            for y in range(3):
                lhs_ref[y, b * channels : (b + 1) * channels, :] = turned

    def load_halo(pieces):
        turned = [piece.T for piece in pieces]
        low = blocks * channels
        half = BLOCK // 2
        for y, other in ((0, turned[1]), (1, None), (2, turned[2])):
            lhs_ref[y, low:, 0:half] = turned[0]
            lhs_ref[y, low:, half:] = jnp.zeros_like(turned[0]) if other is None else other

    load_local(feat)
    def turn_weights(i):
        weight_copies[i].wait()
        for x in range(3):
            weight_t_ref[i, x] = weight_ref[i, x * group * channels : (x + 1) * group * channels, :].T

    turn_weights(0)

    def choose(home, found, value, chosen):
        for i, b in enumerate(chosen):
            value = jnp.where(home == b, found[i * channels : (i + 1) * channels], value)
        return value

    def pick_local(x, carry):
        for j in range(group):
            tap = x * group + j
            found = jnp.dot(
                lhs_ref[0, 0 : blocks * channels], onehot_ref[tap], preferred_element_type=F32
            )
            value = choose(part_ref[tap], found, jnp.zeros((channels, rows), F32), range(blocks))
            picked_ref[tap] = value.astype(BF16)
        return carry

    def convolve(which, picked):
        def add_group(x, total):
            for j in range(group):
                tap = x * group + j
                home = part_ref[tap]
                if picked:
                    found = jnp.dot(
                        lhs_ref[j // 3, blocks * channels :],
                        onehot_ref[tap],
                        preferred_element_type=F32,
                    )
                    value = choose(home, found, picked_ref[tap].astype(F32), (blocks,))
                else:
                    found = jnp.dot(
                        lhs_ref[j // 3], onehot_ref[tap], preferred_element_type=F32
                    )
                    value = choose(
                        home, found, jnp.zeros((channels, rows), F32), range(blocks + 1)
                    )
                picked_ref[tap] = value.astype(BF16)
            taken = picked_ref[pl.ds(x * group, group)].reshape(group * channels, rows)
            return total + jnp.dot(weight_t_ref[which, x], taken, preferred_element_type=F32)

        return add_group

    def tell_sums(which, values):
        kept = values * live
        stats_ref[which, me] = jnp.concatenate(
            [
                jnp.sum(kept, axis=0, keepdims=True),
                jnp.sum(kept * values, axis=0, keepdims=True),
            ],
            axis=0,
        )
        share(which, stats_ref.at[which])

    def affine(which, voxels, gain_ref, shift_ref):
        total = shared(which, stats_ref.at[which])
        average = total[0:1] / voxels
        variance = total[1:2] / voxels - average * average
        scale = lax.rsqrt(variance + EPSILON) * gain_ref[...]
        return lambda values: (values - average) * scale + shift_ref[...]

    lax.fori_loop(0, ahead, pick_local, 0)
    halo(0, False)
    load_halo([halo_ref[i] for i in range(3)])
    blank = jnp.zeros((channels, rows), F32)
    first = lax.fori_loop(0, ahead, convolve(0, True), blank)
    first = lax.fori_loop(ahead, 3, convolve(0, False), first).T
    tell_sums(0, first)
    coarse = first.astype(BF16)
    fine = (first - coarse.astype(F32)).astype(BF16)
    both = jnp.dot(
        face_hot_ref[...],
        jnp.concatenate([coarse, fine], axis=1),
        preferred_element_type=F32,
    )
    wide_send_ref[...] = both[:, 0:channels] + both[:, channels:]
    halo(1, True)
    turn_weights(1)
    for copy in affine_copies:
        copy.wait()
    voxels = shared(2, counts_ref)
    norm_one = affine(0, voxels, gain_one_ref, shift_one_ref)
    load_local((live * jnp.maximum(norm_one(first), 0.0)).astype(BF16))
    halo(1, False)
    load_halo([jnp.maximum(norm_one(wide_halo_ref[i]), 0.0).astype(BF16) for i in range(3)])
    second = lax.fori_loop(0, 3, convolve(1, False), blank).T
    tell_sums(1, second)
    norm_two = affine(1, voxels, gain_two_ref, shift_two_ref)
    summed = norm_two(second) + feat_ref[...].astype(F32)
    out_ref[...] = (live * jnp.maximum(summed, 0.0)).astype(BF16)


def per_device(
    n_slab,
    n_tile,
    features,
    counts,
    rulebook,
    face_rows,
    conv_one,
    gain_one,
    shift_one,
    conv_two,
    gain_two,
    shift_two,
):
    rows, channels = features.shape[2:]
    taps = rulebook.shape[2]
    faces, face_len = face_rows.shape[2:]
    blocks = rows // BLOCK
    smem = pl.BlockSpec(memory_space=pltpu.SMEM)
    vmem = pl.BlockSpec(memory_space=pltpu.VMEM)
    hbm = pl.BlockSpec(memory_space=pltpu.HBM)
    group = taps // 3 * channels
    output = pl.pallas_call(
        partial(block_kernel, n_slab, n_tile),
        out_shape=jax.ShapeDtypeStruct((rows, channels), features.dtype),
        in_specs=[hbm, smem] + [hbm] * 8,
        out_specs=vmem,
        scratch_shapes=[
            pltpu.VMEM((rows, channels), BF16),
            pltpu.VMEM((taps, 1, rows), jnp.int32),
            pltpu.VMEM((faces, face_len), jnp.int32),
            pltpu.VMEM((1, channels), F32),
            pltpu.VMEM((1, channels), F32),
            pltpu.VMEM((1, channels), F32),
            pltpu.VMEM((1, channels), F32),
            pltpu.VMEM((2, taps * channels, channels), BF16),
            pltpu.VMEM((2, 3, channels, group), BF16),
            pltpu.VMEM((taps, BLOCK, rows), BF16),
            pltpu.VMEM((taps, 1, rows), jnp.int32),
            pltpu.VMEM((faces * face_len, rows), BF16),
            pltpu.VMEM((128, 128), F32),
            pltpu.VMEM((faces * face_len, channels), BF16),
            pltpu.VMEM((faces * face_len, channels), F32),
            pltpu.VMEM((3, BLOCK // 2, channels), BF16),
            pltpu.VMEM((3, BLOCK // 2, channels), F32),
            pltpu.VMEM((3, (blocks + 1) * channels, BLOCK), BF16),
            pltpu.VMEM((taps, channels, rows), BF16),
            pltpu.VMEM((2, n_slab * n_tile, 2, channels), F32),
            pltpu.VMEM((n_slab * n_tile, 1, channels), F32),
            pltpu.SemaphoreType.DMA((9,)),
            pltpu.SemaphoreType.DMA((2, 8)),
            pltpu.SemaphoreType.DMA((2, 8)),
            pltpu.SemaphoreType.DMA((3,)),
            pltpu.SemaphoreType.DMA((3,)),
        ],
        compiler_params=pltpu.CompilerParams(
            collective_id=0, has_side_effects=True, vmem_limit_bytes=63200000
        ),
    )(
        features[0, 0],
        counts,
        rulebook.reshape(taps, 1, rows),
        face_rows[0, 0],
        gain_one[None],
        shift_one[None],
        gain_two[None],
        shift_two[None],
        conv_one.reshape(taps * channels, channels),
        conv_two.reshape(taps * channels, channels),
    )
    return output[None, None]


def solution(mesh):
    placed = (
        P("slab", "tile", None, None),
        P("slab", "tile"),
        P("slab", "tile", None, None),
        P("slab", "tile", None, None),
        P(),
        P(),
        P(),
        P(),
        P(),
        P(),
    )
    return jax.shard_map(
        partial(per_device, mesh.shape["slab"], mesh.shape["tile"]),
        mesh=mesh,
        in_specs=placed,
        out_specs=P("slab", "tile", None, None),
        check_vma=False,
    )
```

```python
from functools import partial

import jax
import jax.numpy as jnp
from jax import lax
from jax.experimental import pallas as pl
from jax.experimental.pallas import tpu as pltpu
from jax.sharding import PartitionSpec as P

SIDE = 8
EPSILON = 1e-05
MESH = pl.DeviceIdType.MESH
BLOCK = 256
PIECE = 16
F32 = jnp.float32
BF16 = jnp.bfloat16


def transfers(face_len):
    low, high = 0, face_len
    edge = face_len - PIECE
    end = PIECE + face_len
    return (
        (1, 0, high, face_len, 0, 0),
        (-1, 0, low, face_len, 0, face_len),
        (0, 1, 3 * face_len, face_len, 1, PIECE),
        (0, -1, 2 * face_len, face_len, 2, PIECE),
        (1, 1, high + edge, PIECE, 1, 0),
        (-1, 1, low + edge, PIECE, 1, end),
        (1, -1, high, PIECE, 2, 0),
        (-1, -1, low, PIECE, 2, end),
    )


def block_kernel(
    n_slab,
    n_tile,
    feat_hbm,
    count_ref,
    rule_hbm,
    face_hbm,
    gain_one_hbm,
    shift_one_hbm,
    gain_two_hbm,
    shift_two_hbm,
    conv_one_ref,
    conv_two_ref,
    out_ref,
    feat_ref,
    rule_ref,
    face_ref,
    gain_one_ref,
    shift_one_ref,
    gain_two_ref,
    shift_two_ref,
    weight_ref,
    weight_t_ref,
    onehot_ref,
    part_ref,
    keep_ref,
    face_hot_ref,
    square_ref,
    slope_ref,
    send_ref,
    wide_send_ref,
    halo_ref,
    wide_halo_ref,
    lhs_ref,
    picked_ref,
    stats_ref,
    counts_ref,
    input_sem,
    send_sem,
    recv_sem,
    stat_send_sem,
    stat_recv_sem,
):
    rows, channels = feat_ref.shape
    taps = rule_ref.shape[0]
    face_len = face_ref.shape[1]
    column = face_len // SIDE
    n_dev = n_slab * n_tile
    blocks = rows // BLOCK
    group = taps // 3
    slab = lax.axis_index("slab")
    tile = lax.axis_index("tile")
    me = slab * n_tile + tile

    def fetch(i, src, dst):
        return pltpu.make_async_copy(src, dst, input_sem.at[i])

    input_copies = [
        fetch(0, feat_hbm, feat_ref),
        fetch(1, face_hbm, face_ref),
        fetch(2, rule_hbm, rule_ref),
    ]
    affine_copies = [
        fetch(3, gain_one_hbm, gain_one_ref),
        fetch(4, shift_one_hbm, shift_one_ref),
        fetch(5, gain_two_hbm, gain_two_ref),
        fetch(6, shift_two_hbm, shift_two_ref),
    ]
    weight_copies = [
        fetch(7, conv_one_ref, weight_ref.at[0]),
        fetch(8, conv_two_ref, weight_ref.at[1]),
    ]
    for copy in (input_copies[1], input_copies[0], input_copies[2]):
        copy.start()
    halo_ref[...] = jnp.zeros_like(halo_ref)
    wide_halo_ref[...] = jnp.zeros_like(wide_halo_ref)

    def moved(place, step, size):
        if size & (size - 1) == 0:
            return place ^ step
        place = place + step
        return jnp.where(place >= size, place - size, place)

    def each_peer(act):
        for j in reversed(range(n_tile)):
            other = moved(tile, j, n_tile) if j else tile

            def visit(i, carry):
                act({"slab": moved(slab, n_slab - 1 - i, n_slab), "tile": other})
                return carry

            last = n_slab if j else n_slab - 1
            lax.fori_loop(0, last, visit, 0, unroll=n_slab <= 16)

    barrier = pltpu.get_barrier_semaphore()

    each_peer(
        lambda peer: pl.semaphore_signal(
            barrier, inc=1, device_id=peer, device_id_type=MESH
        )
    )
    for copy in weight_copies + affine_copies:
        copy.start()

    def halo(which, start):
        source, target = ((send_ref, halo_ref), (wide_send_ref, wide_halo_ref))[which]
        for j, (ds, dt, first, size, buffer, place) in enumerate(transfers(face_len)):
            copy = pltpu.make_async_remote_copy(
                src_ref=source.at[pl.ds(first, size)],
                dst_ref=target.at[buffer, pl.ds(place, size)],
                send_sem=send_sem.at[which, j],
                recv_sem=recv_sem.at[which, j],
                device_id={"slab": slab + ds, "tile": tile + dt},
                device_id_type=MESH,
            )
            sends, receives = True, True
            if ds > 0:
                sends, receives = slab < n_slab - 1, slab > 0
            elif ds < 0:
                sends, receives = slab > 0, slab < n_slab - 1
            if dt > 0:
                sends, receives = sends & (tile < n_tile - 1), receives & (tile > 0)
            elif dt < 0:
                sends, receives = sends & (tile > 0), receives & (tile < n_tile - 1)
            if start:
                pl.when(sends)(copy.start)
            else:
                pl.when(receives)(copy.wait_recv)
                pl.when(sends)(copy.wait_send)

    input_copies[1].wait()
    square_ref[...] = jnp.zeros_like(square_ref)
    square_ref[0:4, 0:face_len] = face_ref[...].astype(F32)
    face_cols = square_ref[...].T
    lane_rows = lax.broadcasted_iota(jnp.int32, (face_len, rows), 1)
    for k in range(4):
        wanted = face_cols[0:face_len, k : k + 1].astype(jnp.int32)
        face_hot_ref[k * face_len : (k + 1) * face_len, :] = jnp.where(
            lane_rows == wanted, 1.0, 0.0
        ).astype(BF16)

    input_copies[0].wait()
    feat = feat_ref[...]
    send_ref[...] = jnp.dot(face_hot_ref[...], feat, preferred_element_type=F32).astype(BF16)

    input_copies[2].wait()
    rule = rule_ref[...]
    tile_len = face_len + 2 * column
    below = rows + 2 * face_len
    above = below + tile_len
    q_low = rule - below
    q_high = rule - above
    base = 2 * face_len + PIECE - column
    skip = PIECE - column
    place_low = base + q_low + jnp.where(q_low >= column + face_len, skip, 0)
    place_high = base + q_high - jnp.where(q_high < column, skip, 0)
    place = jnp.where(
        rule < rows,
        rule & (BLOCK - 1),
        jnp.where(
            rule < below, rule - rows, jnp.where(rule < above, place_low, place_high)
        ),
    )
    part = jnp.where(
        rule < rows, rule // BLOCK, jnp.where(rule < above + tile_len, blocks, blocks + 1)
    )
    part_ref[...] = part
    dead = (part > blocks) | ((rule < rows) & (rule >= count_ref[0, 0]))
    keep_ref[...] = jnp.where(dead, 0, 1)
    position = lax.broadcasted_iota(jnp.int32, (BLOCK, rows), 0).astype(F32).astype(BF16)
    place = place.astype(F32).astype(BF16)
    one, none = jnp.ones((BLOCK, rows), BF16), jnp.zeros((BLOCK, rows), BF16)
    for k in range(taps):
        onehot_ref[k] = jnp.where(position == place[k], one, none)

    count = count_ref[0, 0]
    live = (lax.broadcasted_iota(jnp.int32, (rows, 1), 0) < count).astype(F32)

    def share(which, buffer):
        mine = buffer.at[me]
        each_peer(
            lambda peer: pltpu.make_async_remote_copy(
                src_ref=mine,
                dst_ref=mine,
                send_sem=stat_send_sem.at[which],
                recv_sem=stat_recv_sem.at[which],
                device_id=peer,
                device_id_type=MESH,
            ).start()
        )

    def shared(which, buffer):
        others = buffer.at[pl.ds(0, n_dev - 1)]
        pltpu.make_async_copy(others, others, stat_recv_sem.at[which]).wait()
        pltpu.make_async_copy(others, others, stat_send_sem.at[which]).wait()
        return jnp.sum(buffer[...], axis=0)

    counts_ref[me] = jnp.full((1, channels), count.astype(F32))
    pl.semaphore_wait(barrier, n_dev - 1)
    halo(0, True)
    share(2, counts_ref)

    def load_local(values):
        for b in range(blocks):
            turned = values[b * BLOCK : (b + 1) * BLOCK].T
            for y in range(3):
                lhs_ref[y, b * channels : (b + 1) * channels, :] = turned

    def load_halo(pieces):
        turned = [piece.T for piece in pieces]
        low = blocks * channels
        half = BLOCK // 2
        for y, other in ((0, turned[1]), (1, None), (2, turned[2])):
            lhs_ref[y, low:, 0:half] = turned[0]
            lhs_ref[y, low:, half:] = jnp.zeros_like(turned[0]) if other is None else other

    load_local(feat)
    def turn_weights(i):
        weight_copies[i].wait()
        for x in range(3):
            weight_t_ref[i, x] = weight_ref[i, x * group * channels : (x + 1) * group * channels, :].T

    turn_weights(0)

    def choose(home, found, value, chosen):
        for i, b in enumerate(chosen):
            value = jnp.where(home == b, found[i * channels : (i + 1) * channels], value)
        return value

    def pick_local(x, carry):
        for j in range(group):
            tap = x * group + j
            found = jnp.dot(
                lhs_ref[0, 0 : blocks * channels], onehot_ref[tap], preferred_element_type=F32
            )
            value = choose(part_ref[tap], found, jnp.zeros((channels, rows), F32), range(blocks))
            picked_ref[tap] = value.astype(BF16)
        return carry

    def pick_halo(tap, j):
        found = jnp.dot(
            lhs_ref[j // 3, blocks * channels :], onehot_ref[tap], preferred_element_type=F32
        )
        value = choose(part_ref[tap], found, picked_ref[tap].astype(F32), (blocks,))
        picked_ref[tap] = value.astype(BF16)

    def pick_halos(x, carry):
        for j in range(group):
            pick_halo(x * group + j, j)
        return carry

    def multiply(which, x, total):
        taken = picked_ref[pl.ds(x * group, group)].reshape(group * channels, rows)
        return total + jnp.dot(weight_t_ref[which, x], taken, preferred_element_type=F32)

    def convolve_one(x, total):
        pick_halos(x, 0)
        return multiply(0, x, total)

    def tell_sums(which, values):
        kept = values * live
        stats_ref[which, me] = jnp.concatenate(
            [
                jnp.sum(kept, axis=0, keepdims=True),
                jnp.sum(kept * values, axis=0, keepdims=True),
            ],
            axis=0,
        )
        share(which, stats_ref.at[which])
        return stats_ref[which, me][0:1] / count.astype(F32)

    def affine(which, voxels, gain_ref, shift_ref):
        total = shared(which, stats_ref.at[which])
        average = total[0:1] / voxels
        variance = total[1:2] / voxels - average * average
        scale = lax.rsqrt(variance + EPSILON) * gain_ref[...]
        return scale, shift_ref[...] - average * scale

    lax.fori_loop(0, 3, pick_local, 0)
    halo(0, False)
    load_halo([halo_ref[i] for i in range(3)])
    blank = jnp.zeros((channels, rows), F32)
    first = lax.fori_loop(0, 3, convolve_one, blank).T
    centre = tell_sums(0, first)
    coarse = first.astype(BF16)
    fine = (first - coarse.astype(F32)).astype(BF16)
    both = jnp.dot(
        face_hot_ref[...],
        jnp.concatenate([coarse, fine], axis=1),
        preferred_element_type=F32,
    )
    wide_send_ref[...] = both[:, 0:channels] + both[:, channels:]
    halo(1, True)
    load_local((first - centre).astype(BF16))
    lax.fori_loop(0, 3, pick_local, 0)
    halo(1, False)
    load_halo([(wide_halo_ref[i] - centre).astype(BF16) for i in range(3)])
    lax.fori_loop(0, 3, pick_halos, 0)
    turn_weights(1)
    for copy in affine_copies:
        copy.wait()
    voxels = shared(2, counts_ref)
    scale, offset = affine(0, voxels, gain_one_ref, shift_one_ref)

    square_ref[...] = jnp.broadcast_to(scale, (channels, channels)).T
    slope_ref[...] = jnp.broadcast_to(centre * scale + offset, (channels, channels)).T

    def convolve_two(x, total):
        slope = jnp.concatenate([square_ref[...]] * (rows // channels), axis=1)
        level = jnp.concatenate([slope_ref[...]] * (rows // channels), axis=1)
        for j in range(group):
            tap = x * group + j
            value = jnp.maximum(picked_ref[tap].astype(F32) * slope + level, 0.0)
            value = jnp.where(keep_ref[tap] > 0, value, 0.0)
            picked_ref[tap] = value.astype(BF16)
        return multiply(1, x, total)

    second = lax.fori_loop(0, 3, convolve_two, blank).T
    tell_sums(1, second)
    scale, offset = affine(1, voxels, gain_two_ref, shift_two_ref)
    summed = second * scale + offset + feat_ref[...].astype(F32)
    out_ref[...] = (live * jnp.maximum(summed, 0.0)).astype(BF16)


def per_device(
    n_slab,
    n_tile,
    features,
    counts,
    rulebook,
    face_rows,
    conv_one,
    gain_one,
    shift_one,
    conv_two,
    gain_two,
    shift_two,
):
    rows, channels = features.shape[2:]
    taps = rulebook.shape[2]
    faces, face_len = face_rows.shape[2:]
    blocks = rows // BLOCK
    smem = pl.BlockSpec(memory_space=pltpu.SMEM)
    vmem = pl.BlockSpec(memory_space=pltpu.VMEM)
    hbm = pl.BlockSpec(memory_space=pltpu.HBM)
    group = taps // 3 * channels
    output = pl.pallas_call(
        partial(block_kernel, n_slab, n_tile),
        out_shape=jax.ShapeDtypeStruct((rows, channels), features.dtype),
        in_specs=[hbm, smem] + [hbm] * 8,
        out_specs=vmem,
        scratch_shapes=[
            pltpu.VMEM((rows, channels), BF16),
            pltpu.VMEM((taps, 1, rows), jnp.int32),
            pltpu.VMEM((faces, face_len), jnp.int32),
            pltpu.VMEM((1, channels), F32),
            pltpu.VMEM((1, channels), F32),
            pltpu.VMEM((1, channels), F32),
            pltpu.VMEM((1, channels), F32),
            pltpu.VMEM((2, taps * channels, channels), BF16),
            pltpu.VMEM((2, 3, channels, group), BF16),
            pltpu.VMEM((taps, BLOCK, rows), BF16),
            pltpu.VMEM((taps, 1, rows), jnp.int32),
            pltpu.VMEM((taps, 1, rows), jnp.int32),
            pltpu.VMEM((faces * face_len, rows), BF16),
            pltpu.VMEM((channels, channels), F32),
            pltpu.VMEM((channels, channels), F32),
            pltpu.VMEM((faces * face_len, channels), BF16),
            pltpu.VMEM((faces * face_len, channels), F32),
            pltpu.VMEM((3, BLOCK // 2, channels), BF16),
            pltpu.VMEM((3, BLOCK // 2, channels), F32),
            pltpu.VMEM((3, (blocks + 1) * channels, BLOCK), BF16),
            pltpu.VMEM((taps, channels, rows), BF16),
            pltpu.VMEM((2, n_slab * n_tile, 2, channels), F32),
            pltpu.VMEM((n_slab * n_tile, 1, channels), F32),
            pltpu.SemaphoreType.DMA((9,)),
            pltpu.SemaphoreType.DMA((2, 8)),
            pltpu.SemaphoreType.DMA((2, 8)),
            pltpu.SemaphoreType.DMA((3,)),
            pltpu.SemaphoreType.DMA((3,)),
        ],
        compiler_params=pltpu.CompilerParams(
            collective_id=0, has_side_effects=True, vmem_limit_bytes=63200000
        ),
    )(
        features[0, 0],
        counts,
        rulebook.reshape(taps, 1, rows),
        face_rows[0, 0],
        gain_one[None],
        shift_one[None],
        gain_two[None],
        shift_two[None],
        conv_one.reshape(taps * channels, channels),
        conv_two.reshape(taps * channels, channels),
    )
    return output[None, None]


def solution(mesh):
    placed = (
        P("slab", "tile", None, None),
        P("slab", "tile"),
        P("slab", "tile", None, None),
        P("slab", "tile", None, None),
        P(),
        P(),
        P(),
        P(),
        P(),
        P(),
    )
    return jax.shard_map(
        partial(per_device, mesh.shape["slab"], mesh.shape["tile"]),
        mesh=mesh,
        in_specs=placed,
        out_specs=P("slab", "tile", None, None),
        check_vma=False,
    )
```

```python
from functools import partial

import jax
import jax.numpy as jnp
from jax import lax
from jax.experimental import pallas as pl
from jax.experimental.pallas import tpu as pltpu
from jax.sharding import PartitionSpec as P

SIDE = 8
EPSILON = 1e-05
MESH = pl.DeviceIdType.MESH
BLOCK = 256
PIECE = 16
F32 = jnp.float32
BF16 = jnp.bfloat16


def transfers(face_len):
    low, high = 0, face_len
    edge = face_len - PIECE
    end = PIECE + face_len
    return (
        (1, 0, high, face_len, 0, 0),
        (-1, 0, low, face_len, 0, face_len),
        (0, 1, 3 * face_len, face_len, 1, PIECE),
        (0, -1, 2 * face_len, face_len, 2, PIECE),
        (1, 1, high + edge, PIECE, 1, 0),
        (-1, 1, low + edge, PIECE, 1, end),
        (1, -1, high, PIECE, 2, 0),
        (-1, -1, low, PIECE, 2, end),
    )


def block_kernel(
    n_slab,
    n_tile,
    feat_hbm,
    count_ref,
    rule_hbm,
    face_hbm,
    gain_one_hbm,
    shift_one_hbm,
    gain_two_hbm,
    shift_two_hbm,
    conv_one_ref,
    conv_two_ref,
    out_ref,
    feat_ref,
    rule_ref,
    face_ref,
    gain_one_ref,
    shift_one_ref,
    gain_two_ref,
    shift_two_ref,
    weight_ref,
    weight_t_ref,
    onehot_ref,
    part_ref,
    keep_ref,
    face_hot_ref,
    square_ref,
    slope_ref,
    own_ref,
    send_ref,
    wide_send_ref,
    halo_ref,
    wide_halo_ref,
    lhs_ref,
    picked_ref,
    stats_ref,
    counts_ref,
    input_sem,
    send_sem,
    recv_sem,
    stat_send_sem,
    stat_recv_sem,
):
    rows, channels = feat_ref.shape
    taps = rule_ref.shape[0]
    face_len = face_ref.shape[1]
    column = face_len // SIDE
    n_dev = n_slab * n_tile
    blocks = rows // BLOCK
    group = taps // 3
    slab = lax.axis_index("slab")
    tile = lax.axis_index("tile")
    me = slab * n_tile + tile

    def fetch(i, src, dst):
        return pltpu.make_async_copy(src, dst, input_sem.at[i])

    input_copies = [
        fetch(0, feat_hbm, feat_ref),
        fetch(1, face_hbm, face_ref),
        fetch(2, rule_hbm, rule_ref),
    ]
    affine_copies = [
        fetch(3, gain_one_hbm, gain_one_ref),
        fetch(4, shift_one_hbm, shift_one_ref),
        fetch(5, gain_two_hbm, gain_two_ref),
        fetch(6, shift_two_hbm, shift_two_ref),
    ]
    weight_copies = [
        fetch(7, conv_one_ref, weight_ref.at[0]),
        fetch(8, conv_two_ref, weight_ref.at[1]),
    ]
    for copy in (input_copies[1], input_copies[0], input_copies[2]):
        copy.start()
    halo_ref[...] = jnp.zeros_like(halo_ref)
    wide_halo_ref[...] = jnp.zeros_like(wide_halo_ref)

    def moved(place, step, size):
        if size & (size - 1) == 0:
            return place ^ step
        place = place + step
        return jnp.where(place >= size, place - size, place)

    def each_peer(act):
        for j in reversed(range(n_tile)):
            other = moved(tile, j, n_tile) if j else tile

            def visit(i, carry):
                act({"slab": moved(slab, n_slab - 1 - i, n_slab), "tile": other})
                return carry

            last = n_slab if j else n_slab - 1
            lax.fori_loop(0, last, visit, 0, unroll=n_slab <= 16)

    barrier = pltpu.get_barrier_semaphore()

    each_peer(
        lambda peer: pl.semaphore_signal(
            barrier, inc=1, device_id=peer, device_id_type=MESH
        )
    )
    for copy in weight_copies + affine_copies:
        copy.start()

    def halo(which, start):
        source, target = ((send_ref, halo_ref), (wide_send_ref, wide_halo_ref))[which]
        for j, (ds, dt, first, size, buffer, place) in enumerate(transfers(face_len)):
            copy = pltpu.make_async_remote_copy(
                src_ref=source.at[pl.ds(first, size)],
                dst_ref=target.at[buffer, pl.ds(place, size)],
                send_sem=send_sem.at[which, j],
                recv_sem=recv_sem.at[which, j],
                device_id={"slab": slab + ds, "tile": tile + dt},
                device_id_type=MESH,
            )
            sends, receives = True, True
            if ds > 0:
                sends, receives = slab < n_slab - 1, slab > 0
            elif ds < 0:
                sends, receives = slab > 0, slab < n_slab - 1
            if dt > 0:
                sends, receives = sends & (tile < n_tile - 1), receives & (tile > 0)
            elif dt < 0:
                sends, receives = sends & (tile > 0), receives & (tile < n_tile - 1)
            if start:
                pl.when(sends)(copy.start)
            else:
                pl.when(receives)(copy.wait_recv)
                pl.when(sends)(copy.wait_send)

    input_copies[1].wait()
    square_ref[...] = jnp.zeros_like(square_ref)
    square_ref[0:4, 0:face_len] = face_ref[...].astype(F32)
    face_cols = square_ref[...].T
    lane_rows = lax.broadcasted_iota(jnp.int32, (face_len, rows), 1)
    for k in range(4):
        wanted = face_cols[0:face_len, k : k + 1].astype(jnp.int32)
        face_hot_ref[k * face_len : (k + 1) * face_len, :] = jnp.where(
            lane_rows == wanted, 1.0, 0.0
        ).astype(BF16)

    input_copies[0].wait()
    feat = feat_ref[...]
    send_ref[...] = jnp.dot(face_hot_ref[...], feat, preferred_element_type=F32).astype(BF16)

    input_copies[2].wait()
    rule = rule_ref[...]
    tile_len = face_len + 2 * column
    below = rows + 2 * face_len
    above = below + tile_len
    q_low = rule - below
    q_high = rule - above
    base = 2 * face_len + PIECE - column
    skip = PIECE - column
    place_low = base + q_low + jnp.where(q_low >= column + face_len, skip, 0)
    place_high = base + q_high - jnp.where(q_high < column, skip, 0)
    place = jnp.where(
        rule < rows,
        rule & (BLOCK - 1),
        jnp.where(
            rule < below, rule - rows, jnp.where(rule < above, place_low, place_high)
        ),
    )
    part = jnp.where(
        rule < rows, rule // BLOCK, jnp.where(rule < above + tile_len, blocks, blocks + 1)
    )
    part_ref[...] = part
    dead = (part > blocks) | ((rule < rows) & (rule >= count_ref[0, 0]))
    keep_ref[...] = jnp.where(dead, 0, 1)
    position = lax.broadcasted_iota(jnp.int32, (BLOCK, rows), 0).astype(F32).astype(BF16)
    place = place.astype(F32).astype(BF16)
    one, none = jnp.ones((BLOCK, rows), BF16), jnp.zeros((BLOCK, rows), BF16)
    for k in range(taps):
        onehot_ref[k] = jnp.where(position == place[k], one, none)

    count = count_ref[0, 0]
    live = (lax.broadcasted_iota(jnp.int32, (rows, 1), 0) < count).astype(F32)

    def share(which, buffer):
        mine = buffer.at[me]
        each_peer(
            lambda peer: pltpu.make_async_remote_copy(
                src_ref=mine,
                dst_ref=mine,
                send_sem=stat_send_sem.at[which],
                recv_sem=stat_recv_sem.at[which],
                device_id=peer,
                device_id_type=MESH,
            ).start()
        )

    def shared(which, buffer):
        others = buffer.at[pl.ds(0, n_dev - 1)]
        pltpu.make_async_copy(others, others, stat_recv_sem.at[which]).wait()
        pltpu.make_async_copy(others, others, stat_send_sem.at[which]).wait()
        return jnp.sum(buffer[...], axis=0)

    counts_ref[me] = jnp.full((1, channels), count.astype(F32))
    pl.semaphore_wait(barrier, n_dev - 1)
    halo(0, True)
    share(2, counts_ref)

    def load_local(values):
        for b in range(blocks):
            turned = values[b * BLOCK : (b + 1) * BLOCK].T
            for y in range(3):
                lhs_ref[y, b * channels : (b + 1) * channels, :] = turned

    def load_halo(pieces):
        turned = [piece.T for piece in pieces]
        low = blocks * channels
        half = BLOCK // 2
        for y, other in ((0, turned[1]), (1, None), (2, turned[2])):
            lhs_ref[y, low:, 0:half] = turned[0]
            lhs_ref[y, low:, half:] = jnp.zeros_like(turned[0]) if other is None else other

    load_local(feat)
    def turn_weights(i):
        weight_copies[i].wait()
        for x in range(3):
            weight_t_ref[i, x] = weight_ref[i, x * group * channels : (x + 1) * group * channels, :].T

    turn_weights(0)

    def choose(home, found, value, chosen):
        for i, b in enumerate(chosen):
            value = jnp.where(home == b, found[i * channels : (i + 1) * channels], value)
        return value

    def pick_local(x, carry):
        for j in range(group):
            tap = x * group + j
            found = jnp.dot(
                lhs_ref[0, 0 : blocks * channels], onehot_ref[tap], preferred_element_type=F32
            )
            value = choose(part_ref[tap], found, jnp.zeros((channels, rows), F32), range(blocks))
            picked_ref[tap] = value.astype(BF16)
        return carry

    def pick_halos(x):
        for j in range(group):
            tap = x * group + j
            found = jnp.dot(
                lhs_ref[j // 3, blocks * channels :], onehot_ref[tap], preferred_element_type=F32
            )
            value = choose(part_ref[tap], found, picked_ref[tap].astype(F32), (blocks,))
            picked_ref[tap] = value.astype(BF16)

    def multiply(which, x, total):
        taken = picked_ref[pl.ds(x * group, group)].reshape(group * channels, rows)
        return total + jnp.dot(weight_t_ref[which, x], taken, preferred_element_type=F32)

    def convolve_one(x, total):
        pick_halos(x)
        return multiply(0, x, total)

    def tell_sums(which, values):
        kept = values * live
        stats_ref[which, me] = jnp.concatenate(
            [
                jnp.sum(kept, axis=0, keepdims=True),
                jnp.sum(kept * values, axis=0, keepdims=True),
            ],
            axis=0,
        )
        share(which, stats_ref.at[which])
        return stats_ref[which, me][0:1] / count.astype(F32)

    def affine(which, voxels, gain_ref, shift_ref):
        total = shared(which, stats_ref.at[which])
        average = total[0:1] / voxels
        variance = total[1:2] / voxels - average * average
        scale = lax.rsqrt(variance + EPSILON) * gain_ref[...]
        return scale, shift_ref[...] - average * scale

    lax.fori_loop(0, 3, pick_local, 0)
    halo(0, False)
    load_halo([halo_ref[i] for i in range(3)])
    blank = jnp.zeros((channels, rows), F32)
    first = lax.fori_loop(0, 3, convolve_one, blank).T
    centre = tell_sums(0, first)
    coarse = first.astype(BF16)
    fine = (first - coarse.astype(F32)).astype(BF16)
    both = jnp.dot(
        face_hot_ref[...],
        jnp.concatenate([coarse, fine], axis=1),
        preferred_element_type=F32,
    )
    wide_send_ref[...] = both[:, 0:channels] + both[:, channels:]
    halo(1, True)
    centred = first - centre
    for b in range(blocks):
        turned = centred[b * BLOCK : (b + 1) * BLOCK].T
        own_ref[:, b * BLOCK : (b + 1) * BLOCK] = turned
        lhs_ref[0, b * channels : (b + 1) * channels, :] = turned.astype(BF16)
    lax.fori_loop(0, 3, pick_local, 0)
    turn_weights(1)
    for copy in affine_copies:
        copy.wait()
    voxels = shared(2, counts_ref)
    scale, offset = affine(0, voxels, gain_one_ref, shift_one_ref)

    halo(1, False)
    load_halo(
        [
            jnp.maximum(wide_halo_ref[i] * scale + offset, 0.0).astype(BF16)
            for i in range(3)
        ]
    )
    square_ref[...] = jnp.broadcast_to(scale, (channels, channels)).T
    slope_ref[...] = jnp.broadcast_to(centre * scale + offset, (channels, channels)).T

    def convolve_two(x, total):
        slope = jnp.concatenate([square_ref[...]] * (rows // channels), axis=1)
        level = jnp.concatenate([slope_ref[...]] * (rows // channels), axis=1)
        for j in range(group):
            tap = x * group + j
            value = picked_ref[tap].astype(F32)
            if j == group // 2:
                middle = jnp.full((channels, rows), x, jnp.int32) == 1
                value = jnp.where(middle, own_ref[...], value)
            value = jnp.maximum(value * slope + level, 0.0)
            found = jnp.dot(
                lhs_ref[j // 3, blocks * channels :], onehot_ref[tap], preferred_element_type=F32
            )
            value = choose(part_ref[tap], found, value, (blocks,))
            value = jnp.where(keep_ref[tap] > 0, value, 0.0)
            picked_ref[tap] = value.astype(BF16)
        return multiply(1, x, total)

    second = lax.fori_loop(0, 3, convolve_two, blank).T
    tell_sums(1, second)
    scale, offset = affine(1, voxels, gain_two_ref, shift_two_ref)
    summed = second * scale + offset + feat_ref[...].astype(F32)
    out_ref[...] = (live * jnp.maximum(summed, 0.0)).astype(BF16)


def per_device(
    n_slab,
    n_tile,
    features,
    counts,
    rulebook,
    face_rows,
    conv_one,
    gain_one,
    shift_one,
    conv_two,
    gain_two,
    shift_two,
):
    rows, channels = features.shape[2:]
    taps = rulebook.shape[2]
    faces, face_len = face_rows.shape[2:]
    blocks = rows // BLOCK
    smem = pl.BlockSpec(memory_space=pltpu.SMEM)
    vmem = pl.BlockSpec(memory_space=pltpu.VMEM)
    hbm = pl.BlockSpec(memory_space=pltpu.HBM)
    group = taps // 3 * channels
    output = pl.pallas_call(
        partial(block_kernel, n_slab, n_tile),
        out_shape=jax.ShapeDtypeStruct((rows, channels), features.dtype),
        in_specs=[hbm, smem] + [hbm] * 8,
        out_specs=vmem,
        scratch_shapes=[
            pltpu.VMEM((rows, channels), BF16),
            pltpu.VMEM((taps, 1, rows), jnp.int32),
            pltpu.VMEM((faces, face_len), jnp.int32),
            pltpu.VMEM((1, channels), F32),
            pltpu.VMEM((1, channels), F32),
            pltpu.VMEM((1, channels), F32),
            pltpu.VMEM((1, channels), F32),
            pltpu.VMEM((2, taps * channels, channels), BF16),
            pltpu.VMEM((2, 3, channels, group), BF16),
            pltpu.VMEM((taps, BLOCK, rows), BF16),
            pltpu.VMEM((taps, 1, rows), jnp.int32),
            pltpu.VMEM((taps, 1, rows), jnp.int32),
            pltpu.VMEM((faces * face_len, rows), BF16),
            pltpu.VMEM((channels, channels), F32),
            pltpu.VMEM((channels, channels), F32),
            pltpu.VMEM((channels, rows), F32),
            pltpu.VMEM((faces * face_len, channels), BF16),
            pltpu.VMEM((faces * face_len, channels), F32),
            pltpu.VMEM((3, BLOCK // 2, channels), BF16),
            pltpu.VMEM((3, BLOCK // 2, channels), F32),
            pltpu.VMEM((3, (blocks + 1) * channels, BLOCK), BF16),
            pltpu.VMEM((taps, channels, rows), BF16),
            pltpu.VMEM((2, n_slab * n_tile, 2, channels), F32),
            pltpu.VMEM((n_slab * n_tile, 1, channels), F32),
            pltpu.SemaphoreType.DMA((9,)),
            pltpu.SemaphoreType.DMA((2, 8)),
            pltpu.SemaphoreType.DMA((2, 8)),
            pltpu.SemaphoreType.DMA((3,)),
            pltpu.SemaphoreType.DMA((3,)),
        ],
        compiler_params=pltpu.CompilerParams(
            collective_id=0, has_side_effects=True, vmem_limit_bytes=63200000
        ),
    )(
        features[0, 0],
        counts,
        rulebook.reshape(taps, 1, rows),
        face_rows[0, 0],
        gain_one[None],
        shift_one[None],
        gain_two[None],
        shift_two[None],
        conv_one.reshape(taps * channels, channels),
        conv_two.reshape(taps * channels, channels),
    )
    return output[None, None]


def solution(mesh):
    placed = (
        P("slab", "tile", None, None),
        P("slab", "tile"),
        P("slab", "tile", None, None),
        P("slab", "tile", None, None),
        P(),
        P(),
        P(),
        P(),
        P(),
        P(),
    )
    return jax.shard_map(
        partial(per_device, mesh.shape["slab"], mesh.shape["tile"]),
        mesh=mesh,
        in_specs=placed,
        out_specs=P("slab", "tile", None, None),
        check_vma=False,
    )
```

```python
from functools import partial

import jax
import jax.numpy as jnp
from jax import lax
from jax.experimental import pallas as pl
from jax.experimental.pallas import tpu as pltpu
from jax.sharding import PartitionSpec as P

SIDE = 8
EPSILON = 1e-05
MESH = pl.DeviceIdType.MESH
BLOCK = 256
PIECE = 16
F32 = jnp.float32
BF16 = jnp.bfloat16


def transfers(face_len):
    low, high = 0, face_len
    edge = face_len - PIECE
    end = PIECE + face_len
    return (
        (1, 0, high, face_len, 0, 0),
        (-1, 0, low, face_len, 0, face_len),
        (0, 1, 3 * face_len, face_len, 1, PIECE),
        (0, -1, 2 * face_len, face_len, 2, PIECE),
        (1, 1, high + edge, PIECE, 1, 0),
        (-1, 1, low + edge, PIECE, 1, end),
        (1, -1, high, PIECE, 2, 0),
        (-1, -1, low, PIECE, 2, end),
    )


def block_kernel(
    n_slab,
    n_tile,
    feat_hbm,
    count_ref,
    rule_hbm,
    face_hbm,
    gain_one_hbm,
    shift_one_hbm,
    gain_two_hbm,
    shift_two_hbm,
    conv_one_ref,
    conv_two_ref,
    out_ref,
    feat_ref,
    rule_ref,
    face_ref,
    gain_one_ref,
    shift_one_ref,
    gain_two_ref,
    shift_two_ref,
    weight_ref,
    weight_t_ref,
    onehot_ref,
    part_ref,
    keep_ref,
    face_hot_ref,
    square_ref,
    slope_ref,
    own_ref,
    send_ref,
    wide_send_ref,
    halo_ref,
    wide_halo_ref,
    lhs_ref,
    picked_ref,
    stats_ref,
    counts_ref,
    input_sem,
    send_sem,
    recv_sem,
    stat_send_sem,
    stat_recv_sem,
):
    rows, channels = feat_ref.shape
    taps = rule_ref.shape[0]
    face_len = face_ref.shape[1]
    column = face_len // SIDE
    n_dev = n_slab * n_tile
    blocks = rows // BLOCK
    group = taps // 3
    slab = lax.axis_index("slab")
    tile = lax.axis_index("tile")
    me = slab * n_tile + tile

    def fetch(i, src, dst):
        return pltpu.make_async_copy(src, dst, input_sem.at[i])

    input_copies = [
        fetch(0, feat_hbm, feat_ref),
        fetch(1, face_hbm, face_ref),
        fetch(2, rule_hbm, rule_ref),
    ]
    affine_copies = [
        fetch(3, gain_one_hbm, gain_one_ref),
        fetch(4, shift_one_hbm, shift_one_ref),
        fetch(5, gain_two_hbm, gain_two_ref),
        fetch(6, shift_two_hbm, shift_two_ref),
    ]
    weight_copies = [
        fetch(7, conv_one_ref, weight_ref.at[0]),
        fetch(8, conv_two_ref, weight_ref.at[1]),
    ]
    for copy in (input_copies[1], input_copies[0], input_copies[2]):
        copy.start()
    halo_ref[...] = jnp.zeros_like(halo_ref)
    wide_halo_ref[...] = jnp.zeros_like(wide_halo_ref)

    def moved(place, step, size):
        if size & (size - 1) == 0:
            return place ^ step
        place = place + step
        return jnp.where(place >= size, place - size, place)

    def each_peer(act):
        for j in reversed(range(n_tile)):
            other = moved(tile, j, n_tile) if j else tile

            def visit(i, carry):
                act({"slab": moved(slab, n_slab - 1 - i, n_slab), "tile": other})
                return carry

            last = n_slab if j else n_slab - 1
            lax.fori_loop(0, last, visit, 0, unroll=n_slab <= 16)

    barrier = pltpu.get_barrier_semaphore()

    each_peer(
        lambda peer: pl.semaphore_signal(
            barrier, inc=1, device_id=peer, device_id_type=MESH
        )
    )
    for copy in weight_copies + affine_copies:
        copy.start()

    def halo(which, start):
        source, target = ((send_ref, halo_ref), (wide_send_ref, wide_halo_ref))[which]
        for j, (ds, dt, first, size, buffer, place) in enumerate(transfers(face_len)):
            copy = pltpu.make_async_remote_copy(
                src_ref=source.at[pl.ds(first, size)],
                dst_ref=target.at[buffer, pl.ds(place, size)],
                send_sem=send_sem.at[which, j],
                recv_sem=recv_sem.at[which, j],
                device_id={"slab": slab + ds, "tile": tile + dt},
                device_id_type=MESH,
            )
            sends, receives = True, True
            if ds > 0:
                sends, receives = slab < n_slab - 1, slab > 0
            elif ds < 0:
                sends, receives = slab > 0, slab < n_slab - 1
            if dt > 0:
                sends, receives = sends & (tile < n_tile - 1), receives & (tile > 0)
            elif dt < 0:
                sends, receives = sends & (tile > 0), receives & (tile < n_tile - 1)
            if start:
                pl.when(sends)(copy.start)
            else:
                pl.when(receives)(copy.wait_recv)
                pl.when(sends)(copy.wait_send)

    input_copies[1].wait()
    square_ref[...] = jnp.zeros_like(square_ref)
    square_ref[0:4, 0:face_len] = face_ref[...].astype(F32)
    face_cols = square_ref[...].T
    lane_rows = lax.broadcasted_iota(jnp.int32, (face_len, rows), 1)
    for k in range(4):
        wanted = face_cols[0:face_len, k : k + 1].astype(jnp.int32)
        face_hot_ref[k * face_len : (k + 1) * face_len, :] = jnp.where(
            lane_rows == wanted, 1.0, 0.0
        ).astype(BF16)

    input_copies[0].wait()
    feat = feat_ref[...]
    send_ref[...] = jnp.dot(face_hot_ref[...], feat, preferred_element_type=F32).astype(BF16)

    input_copies[2].wait()
    rule = rule_ref[...]
    tile_len = face_len + 2 * column
    below = rows + 2 * face_len
    above = below + tile_len
    q_low = rule - below
    q_high = rule - above
    base = 2 * face_len + PIECE - column
    skip = PIECE - column
    place_low = base + q_low + jnp.where(q_low >= column + face_len, skip, 0)
    place_high = base + q_high - jnp.where(q_high < column, skip, 0)
    place = jnp.where(
        rule < rows,
        rule & (BLOCK - 1),
        jnp.where(
            rule < below, rule - rows, jnp.where(rule < above, place_low, place_high)
        ),
    )
    part = jnp.where(
        rule < rows, rule // BLOCK, jnp.where(rule < above + tile_len, blocks, blocks + 1)
    )
    part_ref[...] = part
    dead = (part > blocks) | ((rule < rows) & (rule >= count_ref[0, 0]))
    keep_ref[...] = jnp.where(dead, 0, 1)
    position = lax.broadcasted_iota(jnp.int32, (BLOCK, rows), 0).astype(F32).astype(BF16)
    place = place.astype(F32).astype(BF16)
    one, none = jnp.ones((BLOCK, rows), BF16), jnp.zeros((BLOCK, rows), BF16)
    for k in range(taps):
        onehot_ref[k] = jnp.where(position == place[k], one, none)

    count = count_ref[0, 0]
    live = (lax.broadcasted_iota(jnp.int32, (rows, 1), 0) < count).astype(F32)

    def share(which, buffer):
        mine = buffer.at[me]
        each_peer(
            lambda peer: pltpu.make_async_remote_copy(
                src_ref=mine,
                dst_ref=mine,
                send_sem=stat_send_sem.at[which],
                recv_sem=stat_recv_sem.at[which],
                device_id=peer,
                device_id_type=MESH,
            ).start()
        )

    def shared(which, buffer):
        others = buffer.at[pl.ds(0, n_dev - 1)]
        pltpu.make_async_copy(others, others, stat_recv_sem.at[which]).wait()
        pltpu.make_async_copy(others, others, stat_send_sem.at[which]).wait()
        return jnp.sum(buffer[...], axis=0)

    counts_ref[me] = jnp.full((1, channels), count.astype(F32))
    pl.semaphore_wait(barrier, n_dev - 1)
    halo(0, True)
    share(2, counts_ref)

    def load_local(values):
        for b in range(blocks):
            turned = values[b * BLOCK : (b + 1) * BLOCK].T
            for y in range(3):
                lhs_ref[y, b * channels : (b + 1) * channels, :] = turned

    def load_halo(pieces):
        turned = [piece.T for piece in pieces]
        low = blocks * channels
        half = BLOCK // 2
        for y, other in ((0, turned[1]), (1, None), (2, turned[2])):
            lhs_ref[y, low:, 0:half] = turned[0]
            lhs_ref[y, low:, half:] = jnp.zeros_like(turned[0]) if other is None else other

    load_local(feat)
    def turn_weights(i):
        weight_copies[i].wait()
        for x in range(3):
            weight_t_ref[i, x] = weight_ref[i, x * group * channels : (x + 1) * group * channels, :].T

    turn_weights(0)

    def choose(home, found, value, chosen):
        for i, b in enumerate(chosen):
            value = jnp.where(home == b, found[i * channels : (i + 1) * channels], value)
        return value

    def pick_local(x, carry):
        for j in range(group):
            tap = x * group + j
            found = jnp.dot(
                lhs_ref[0, 0 : blocks * channels], onehot_ref[tap], preferred_element_type=F32
            )
            value = choose(part_ref[tap], found, jnp.zeros((channels, rows), F32), range(blocks))
            picked_ref[tap] = value.astype(BF16)
        return carry

    def pick_halo(tap, j):
        found = jnp.dot(
            lhs_ref[j // 3, blocks * channels :], onehot_ref[tap], preferred_element_type=F32
        )
        value = choose(part_ref[tap], found, picked_ref[tap].astype(F32), (blocks,))
        picked_ref[tap] = value.astype(BF16)

    def pick_halos(x):
        for j in range(group):
            if x != 1 or j // 3 != 1:
                pick_halo(x * group + j, j)

    def multiply(which, x, total):
        taken = picked_ref[pl.ds(x * group, group)].reshape(group * channels, rows)
        return total + jnp.dot(weight_t_ref[which, x], taken, preferred_element_type=F32)

    def tell_sums(which, values):
        kept = values * live
        stats_ref[which, me] = jnp.concatenate(
            [
                jnp.sum(kept, axis=0, keepdims=True),
                jnp.sum(kept * values, axis=0, keepdims=True),
            ],
            axis=0,
        )
        share(which, stats_ref.at[which])
        return stats_ref[which, me][0:1] / count.astype(F32)

    def affine(which, voxels, gain_ref, shift_ref):
        total = shared(which, stats_ref.at[which])
        average = total[0:1] / voxels
        variance = total[1:2] / voxels - average * average
        scale = lax.rsqrt(variance + EPSILON) * gain_ref[...]
        return scale, shift_ref[...] - average * scale

    lax.fori_loop(0, 3, pick_local, 0)
    halo(0, False)
    load_halo([halo_ref[i] for i in range(3)])
    blank = jnp.zeros((channels, rows), F32)
    first = blank
    for x in range(3):
        pick_halos(x)
        first = multiply(0, x, first)
    first = first.T
    centre = tell_sums(0, first)
    coarse = first.astype(BF16)
    fine = (first - coarse.astype(F32)).astype(BF16)
    both = jnp.dot(
        face_hot_ref[...],
        jnp.concatenate([coarse, fine], axis=1),
        preferred_element_type=F32,
    )
    wide_send_ref[...] = both[:, 0:channels] + both[:, channels:]
    halo(1, True)
    centred = first - centre
    for b in range(blocks):
        turned = centred[b * BLOCK : (b + 1) * BLOCK].T
        own_ref[:, b * BLOCK : (b + 1) * BLOCK] = turned
        lhs_ref[0, b * channels : (b + 1) * channels, :] = turned.astype(BF16)
    lax.fori_loop(0, 3, pick_local, 0)
    turn_weights(1)
    halo(1, False)
    load_halo([(wide_halo_ref[i] - centre).astype(BF16) for i in range(3)])
    for x in range(3):
        pick_halos(x)
    for copy in affine_copies:
        copy.wait()
    voxels = shared(2, counts_ref)
    scale, offset = affine(0, voxels, gain_one_ref, shift_one_ref)

    square_ref[...] = jnp.broadcast_to(scale, (channels, channels)).T
    slope_ref[...] = jnp.broadcast_to(centre * scale + offset, (channels, channels)).T

    def convolve_two(x, total):
        slope = jnp.concatenate([square_ref[...]] * (rows // channels), axis=1)
        level = jnp.concatenate([slope_ref[...]] * (rows // channels), axis=1)
        for j in range(group):
            tap = x * group + j
            value = picked_ref[tap].astype(F32)
            if j == group // 2:
                middle = jnp.full((channels, rows), x, jnp.int32) == 1
                value = jnp.where(middle, own_ref[...], value)
            value = jnp.maximum(value * slope + level, 0.0)
            value = jnp.where(keep_ref[tap] > 0, value, 0.0)
            picked_ref[tap] = value.astype(BF16)
        return multiply(1, x, total)

    second = lax.fori_loop(0, 3, convolve_two, blank).T
    tell_sums(1, second)
    scale, offset = affine(1, voxels, gain_two_ref, shift_two_ref)
    summed = second * scale + offset + feat_ref[...].astype(F32)
    out_ref[...] = (live * jnp.maximum(summed, 0.0)).astype(BF16)


def per_device(
    n_slab,
    n_tile,
    features,
    counts,
    rulebook,
    face_rows,
    conv_one,
    gain_one,
    shift_one,
    conv_two,
    gain_two,
    shift_two,
):
    rows, channels = features.shape[2:]
    taps = rulebook.shape[2]
    faces, face_len = face_rows.shape[2:]
    blocks = rows // BLOCK
    smem = pl.BlockSpec(memory_space=pltpu.SMEM)
    vmem = pl.BlockSpec(memory_space=pltpu.VMEM)
    hbm = pl.BlockSpec(memory_space=pltpu.HBM)
    group = taps // 3 * channels
    output = pl.pallas_call(
        partial(block_kernel, n_slab, n_tile),
        out_shape=jax.ShapeDtypeStruct((rows, channels), features.dtype),
        in_specs=[hbm, smem] + [hbm] * 8,
        out_specs=vmem,
        scratch_shapes=[
            pltpu.VMEM((rows, channels), BF16),
            pltpu.VMEM((taps, 1, rows), jnp.int32),
            pltpu.VMEM((faces, face_len), jnp.int32),
            pltpu.VMEM((1, channels), F32),
            pltpu.VMEM((1, channels), F32),
            pltpu.VMEM((1, channels), F32),
            pltpu.VMEM((1, channels), F32),
            pltpu.VMEM((2, taps * channels, channels), BF16),
            pltpu.VMEM((2, 3, channels, group), BF16),
            pltpu.VMEM((taps, BLOCK, rows), BF16),
            pltpu.VMEM((taps, 1, rows), jnp.int32),
            pltpu.VMEM((taps, 1, rows), jnp.int32),
            pltpu.VMEM((faces * face_len, rows), BF16),
            pltpu.VMEM((channels, channels), F32),
            pltpu.VMEM((channels, channels), F32),
            pltpu.VMEM((channels, rows), F32),
            pltpu.VMEM((faces * face_len, channels), BF16),
            pltpu.VMEM((faces * face_len, channels), F32),
            pltpu.VMEM((3, BLOCK // 2, channels), BF16),
            pltpu.VMEM((3, BLOCK // 2, channels), F32),
            pltpu.VMEM((3, (blocks + 1) * channels, BLOCK), BF16),
            pltpu.VMEM((taps, channels, rows), BF16),
            pltpu.VMEM((2, n_slab * n_tile, 2, channels), F32),
            pltpu.VMEM((n_slab * n_tile, 1, channels), F32),
            pltpu.SemaphoreType.DMA((9,)),
            pltpu.SemaphoreType.DMA((2, 8)),
            pltpu.SemaphoreType.DMA((2, 8)),
            pltpu.SemaphoreType.DMA((3,)),
            pltpu.SemaphoreType.DMA((3,)),
        ],
        compiler_params=pltpu.CompilerParams(
            collective_id=0, has_side_effects=True, vmem_limit_bytes=63200000
        ),
    )(
        features[0, 0],
        counts,
        rulebook.reshape(taps, 1, rows),
        face_rows[0, 0],
        gain_one[None],
        shift_one[None],
        gain_two[None],
        shift_two[None],
        conv_one.reshape(taps * channels, channels),
        conv_two.reshape(taps * channels, channels),
    )
    return output[None, None]


def solution(mesh):
    placed = (
        P("slab", "tile", None, None),
        P("slab", "tile"),
        P("slab", "tile", None, None),
        P("slab", "tile", None, None),
        P(),
        P(),
        P(),
        P(),
        P(),
        P(),
    )
    return jax.shard_map(
        partial(per_device, mesh.shape["slab"], mesh.shape["tile"]),
        mesh=mesh,
        in_specs=placed,
        out_specs=P("slab", "tile", None, None),
        check_vma=False,
    )
```
